512 devices in a mesh: tm: 4 (over y), row: 16 (over z), col: 8 (over x, core).
Axes of the slice: x: 4, y: 4, z: 16, core: 2. Of those that a mesh axis runs over, the one named last changes fastest.
Arguments:
- noisy_video: float32 [16, 2048, 2048], P('tm', 'row', 'col'), may hold values from -6 to 6
- fidelity: float32 [16, 2048, 2048], P('tm', 'row', 'col'), may hold values from 0.5 to 12, as said below
Outputs:
- denoised: float32 [16, 2048, 2048], P('tm', 'row', 'col')
- gaps: float32 [3], replicated
The draws below stay inside these ranges and needn't reach their ends.
Inputs may be any that keep to these rules, and one draw needn't show every extreme that they name: `fidelity`: positive, larger on average toward later rows.
All inputs are finite; a program needn't handle non-finite values.
Results may differ from the reference program's by a relative error of at most 0.0001.
Values sent between devices are 32-bit elements; how exact they have to be, the bound alone decides.
A program may use at most 64 MiB of HBM per device.

```python
import math
import jax
import jax.numpy as jnp
from jax import lax

ITERS = 3
NT = 16
NH = 2048
NW = 2048


def draw_fidelity(key, part):
    inner = jax.random.fold_in(key, 11)
    base = jnp.exp(jax.random.uniform(inner, (NT, NH, NW), jnp.float32, math.log(0.5), math.log(4.0)))
    ramp = jnp.power(3.0, jnp.arange(NH, dtype=jnp.float32) / float(NH))
    return (base * ramp[None, :, None]).astype(jnp.float32)


def shard_levels(stream_key, dims, split, smallest, top_value):
    def one(dim, shards_of):
        steps = jax.random.uniform(jax.random.fold_in(jax.random.fold_in(stream_key, 6), dim), (shards_of,), jnp.float32, smallest / len(split), top_value / len(split))
        return jnp.repeat(jnp.exp(steps), dims[dim] // shards_of).reshape((-1,) + (1,) * (len(dims) - dim - 1))

    loudness = one(*split[0])
    for cut in split[1:]:
        loudness = loudness * one(*cut)
    return loudness


def normal_values(rng, dims, width, bound, cuts=(), kind=jnp.bfloat16):
    factor_of = shard_levels(rng, dims, cuts, -0.22, 0.18) if cuts else 1.0
    drawn = jax.random.normal(rng, dims, jnp.float32) * width * factor_of
    return jnp.minimum(jnp.maximum(drawn, -bound), bound).astype(kind)


def setup_inputs(seed: int = 0) -> dict:
    splits = jax.random.split(jax.random.key(seed), 3)
    noisy_video = normal_values(splits[0], (NT, NH, NW), 1.0, 6.0, ((0, 4), (1, 16), (2, 8)), jnp.float32)
    fidelity = draw_fidelity(jax.random.fold_in(splits[2], 71), 0)
    return dict(noisy_video=noisy_video, fidelity=fidelity)


sigma_step = 0.28
tau_step = 0.28

def forward(field, axis):
    count = field.shape[axis]
    ahead = lax.slice_in_dim(field, 1, count, axis=axis) - lax.slice_in_dim(field, 0, count - 1, axis=axis)
    edge = jnp.zeros_like(lax.slice_in_dim(field, 0, 1, axis=axis))
    return jnp.concatenate([ahead, edge], axis=axis)

def backward(comp, axis):
    count = comp.shape[axis]
    edge = jnp.zeros_like(lax.slice_in_dim(comp, 0, 1, axis=axis))
    before = jnp.concatenate([edge, lax.slice_in_dim(comp, 0, count - 1, axis=axis)], axis=axis)
    return comp - before

def reference(noisy_video, fidelity):
    field = noisy_video
    ubar_field = noisy_video
    zero_field = jnp.zeros_like(noisy_video)
    duals = [zero_field, zero_field, zero_field]
    grad_u = None
    gap_list = []
    for iteration in range(ITERS):
        grads = [forward(ubar_field, 0), forward(ubar_field, 1), forward(ubar_field, 2)]
        if iteration == 0:
            grad_u = grads
        else:
            grad_u = [0.5 * (grads[0] + grad_u[0]), 0.5 * (grads[1] + grad_u[1]), 0.5 * (grads[2] + grad_u[2])]
        moved = [duals[0] + sigma_step * grads[0], duals[1] + sigma_step * grads[1], duals[2] + sigma_step * grads[2]]
        length = jnp.sqrt(moved[0] * moved[0] + moved[1] * moved[1] + moved[2] * moved[2])
        scale = jnp.maximum(1.0, length)
        duals = [moved[0] / scale, moved[1] / scale, moved[2] / scale]
        diverge = backward(duals[0], 0) + backward(duals[1], 1) + backward(duals[2], 2)
        total_var = jnp.sqrt(grad_u[0] * grad_u[0] + grad_u[1] * grad_u[1] + grad_u[2] * grad_u[2])
        resid = field - noisy_video
        term = 0.5 * fidelity * resid * resid + total_var + diverge * diverge / (2.0 * fidelity) + noisy_video * diverge
        gap_list.append(jnp.sum(term) / float(term.size))
        new_field = (field + tau_step * diverge + tau_step * fidelity * noisy_video) / (1.0 + tau_step * fidelity)
        ubar_field = 2.0 * new_field - field
        field = new_field
    return (field, jnp.stack(gap_list).astype(jnp.float32))
```

```python
import functools

import jax
import jax.numpy as jnp
from jax import lax
from jax.experimental import pallas as pl
from jax.experimental.pallas import tpu as pltpu
from jax.sharding import PartitionSpec as P

ITERS = 3
SIGMA = 0.28
TAU = 0.28
TINY = 1.1754943508222875e-38
MESH = pl.DeviceIdType.MESH
F32 = jnp.float32

GROUPS = 16

FRAME_UP, FRAME_DOWN = (1, 0, 0), (-1, 0, 0)
ROW_UP, ROW_DOWN = (0, 1, 0), (0, -1, 0)
COL_UP, COL_DOWN = (0, 0, 1), (0, 0, -1)
NEIGHBOURS = (
    FRAME_UP, FRAME_DOWN, ROW_UP, ROW_DOWN, COL_UP, COL_DOWN,
    (1, -1, 0), (-1, 1, 0), (1, 0, -1), (-1, 0, 1), (0, 1, -1), (0, -1, 1),
)

CHUNKS = ([(0, 16)], [(0, 16)], [(0, 16)])
DUAL_STEPS = ([(0, 16)], [(0, 16)], [(0, 16)])
PRIMAL_STEPS = ([[(0, 16)]], [[(0, 16)]], [[(0, 16)]])


def rows_of(group):
    return pl.ds(pl.multiple_of(8 + 8 * group, 8), 8)


def kernel(
    sizes, f_hbm, fid_hbm, out_hbm, gaps_ref,
    ub, p, gu, res, damp, inv_fid, fid, out_v, c0, c255, cn, cp, tcn, tcp, rcn, rcp, pc, part, plane, part2, line,
    load_sem, out_sem,
    fr_send, fr_recv, row_send, row_recv, col_send, col_recv, tr_send, tr_recv, tc_send, tc_recv, rc_send, rc_recv,
    ar_send, ar_recv,
):
    n_tm, n_row, n_col = sizes
    at = (lax.axis_index("tm"), lax.axis_index("row"), lax.axis_index("col"))

    def there(step):
        return dict(tm=at[0] + step[0], row=at[1] + step[1], col=at[2] + step[2])

    def exists(step):
        found = None
        for pos, size, move in zip(at, sizes, step):
            if move:
                ok = pos < size - 1 if move > 0 else pos > 0
                found = ok if found is None else jnp.logical_and(found, ok)
        return found

    lane = lax.broadcasted_iota(jnp.int32, (8, 128), 1)
    sublane = lax.broadcasted_iota(jnp.int32, (8, 128), 0)
    first_lane, last_lane = lane == 0, lane == 127
    first_row, first_col, first_tm = at[1] == 0, at[2] == 0, at[0] == 0
    last_row, last_col, last_tm = at[1] == n_row - 1, at[2] == n_col - 1, at[0] == n_tm - 1
    edge_lane = jnp.logical_and(last_lane, last_col)

    loads = []
    for h in range(2):
        cols = pl.ds(128 * h, 128)
        loads.append(pltpu.make_async_copy(f_hbm.at[:, :, cols], ub.at[0, 1:5, h, 8:136, :], load_sem.at[h]))
        loads.append(pltpu.make_async_copy(fid_hbm.at[:, :, cols], fid.at[:, h], load_sem.at[2 + h]))
    for load in (loads[0], loads[2], loads[1], loads[3]):
        load.start()

    barrier = pltpu.get_barrier_semaphore()
    arrivals = (n_tm * n_col - 1) + (n_row - 1)
    for step in NEIGHBOURS:
        ok = exists(step)

        @pl.when(ok)
        def _():
            pl.semaphore_signal(barrier, inc=1, device_id=there(step), device_id_type=MESH)

        arrivals = arrivals + ok.astype(jnp.int32)

    def plane_mate(j):
        return dict(tm=lax.rem(at[0] + j // n_col, n_tm), row=at[1], col=lax.rem(at[2] + lax.rem(j, n_col), n_col))

    def line_mate(j):
        return dict(tm=at[0], row=lax.rem(at[1] + j, n_row), col=at[2])

    @pl.loop(1, n_tm * n_col)
    def _(j):
        pl.semaphore_signal(barrier, inc=1, device_id=plane_mate(j), device_id_type=MESH)

    @pl.loop(1, n_row)
    def _(j):
        pl.semaphore_signal(barrier, inc=1, device_id=line_mate(j), device_id_type=MESH)

    zero = jnp.zeros((8, 128), F32)
    p[...] = jnp.zeros_like(p)

    def remote(src, dst, send, recv, step):
        return pltpu.make_async_remote_copy(
            src_ref=src, dst_ref=dst, send_sem=send, recv_sem=recv, device_id=there(step), device_id_type=MESH
        )

    def frame_copies(k, c):
        g0, g1 = CHUNKS[k][c]
        out = []
        rows = pl.ds(8 + 8 * g0, 8 * (g1 - g0))
        for i, (step, src, dst) in enumerate(((FRAME_DOWN, 1, 5), (FRAME_UP, 4, 0))):
            out.append((step, remote(
                ub.at[k, src, :, rows, :], ub.at[k, dst, :, rows, :], fr_send.at[k, c, i], fr_recv.at[k, c, i], step)))
        return out

    def row_copies(k):
        out = []
        low, high = pl.ds(8, 8), pl.ds(128, 8)
        ghost_low, ghost_high = pl.ds(0, 8), pl.ds(136, 8)
        for i, (step, src, dst) in enumerate(((ROW_DOWN, low, ghost_high), (ROW_UP, high, ghost_low))):
            out.append((step, remote(
                ub.at[k, 1:5, :, src, :], ub.at[k, 1:5, :, dst, :], row_send.at[k, i], row_recv.at[k, i], step)))
        out.append(((1, -1, 0), remote(
            ub.at[k, 4, :, low, :], ub.at[k, 0, :, ghost_high, :], tr_send.at[k, 0], tr_recv.at[k, 0], (1, -1, 0))))
        out.append(((-1, 1, 0), remote(
            ub.at[k, 1, :, high, :], ub.at[k, 5, :, ghost_low, :], tr_send.at[k, 1], tr_recv.at[k, 1], (-1, 1, 0))))
        return out

    def col_copies(k, c):
        return [
            (COL_DOWN, remote(c0.at[k, c], cn.at[k, c], col_send.at[k, c, 0], col_recv.at[k, c, 0], COL_DOWN)),
            (COL_UP, remote(c255.at[k, c], cp.at[k, c], col_send.at[k, c, 1], col_recv.at[k, c, 1], COL_UP)),
            ((1, 0, -1), remote(c0.at[k, c], tcn.at[k, c], tc_send.at[k, c, 0], tc_recv.at[k, c, 0], (1, 0, -1))),
            ((-1, 0, 1), remote(c255.at[k, c], tcp.at[k, c], tc_send.at[k, c, 1], tc_recv.at[k, c, 1], (-1, 0, 1))),
        ]

    def corner_copies(k):
        c = len(CHUNKS[k]) - 1
        return [
            ((0, 1, -1), remote(c0.at[k, c], rcn.at[k], rc_send.at[k, 0], rc_recv.at[k, 0], (0, 1, -1))),
            ((0, -1, 1), remote(c255.at[k, c], rcp.at[k], rc_send.at[k, 1], rc_recv.at[k, 1], (0, -1, 1))),
        ]

    def start(copies):
        for step, copy in copies:
            @pl.when(exists(step))
            def _():
                copy.start()

    def wait_sent(copies):
        for step, copy in copies:
            @pl.when(exists(step))
            def _():
                copy.wait_send()

    def wait_received(copies):
        for step, copy in copies:
            @pl.when(exists(tuple(-s for s in step)))
            def _():
                copy.wait_recv()

    def all_copies(k):
        out = row_copies(k) + corner_copies(k)
        for c in range(len(CHUNKS[k])):
            out += frame_copies(k, c) + col_copies(k, c)
        return out

    def packed_at(t, g):
        return (t - 1) * 16 + g

    def packed(x0, x1, t, g, held):
        i = packed_at(t, g)
        here = lane == i
        return (
            jnp.where(here, pltpu.roll(x0, i, 1), held[0]),
            jnp.where(here, pltpu.roll(x1, i + 1, 1), held[1]),
        )

    def pack_first():
        def body(g, held):
            for t in range(1, 5):
                held = packed(ub[0, t, 0, rows_of(g), :], ub[0, t, 1, rows_of(g), :], t, g, held)
            return held

        return lax.fori_loop(0, GROUPS, body, (zero, zero))

    def project(k, m, g):
        if k == 0:
            square = g[0] * g[0] + g[1] * g[1] + g[2] * g[2]
            root = lax.rsqrt(jnp.maximum(square, TINY))
            scale = jnp.minimum(SIGMA, root)
            return [g[d] * scale for d in range(3)], square * root
        square = m[0] * m[0] + m[1] * m[1] + m[2] * m[2]
        scale = lax.rsqrt(jnp.maximum(square, 1.0))
        return [m[d] * scale for d in range(3)], None

    def dual_group(k, rows, below, frames, ghost_of, total):
        x = [[ub[k, t, h, rows, :] for h in range(2)] for t in range(frames[0], 6)]
        for t in frames:
            here, later = x[t - frames[0]], x[t - frames[0] + 1]
            rolled = [pltpu.roll(here[h], 127, 1) for h in range(2)]
            after = [
                jnp.where(last_lane, rolled[1], rolled[0]),
                jnp.where(edge_lane, here[1], jnp.where(last_lane, ghost_of(t), rolled[1])),
            ]
            for h in range(2):
                g = [later[h] - here[h], ub[k, t, h, below, :] - here[h], after[h] - here[h]]
                m = None if k == 0 else [p[d, t, h, rows, :] + SIGMA * g[d] for d in range(3)]
                new, length = project(k, m, g)
                for d in range(3):
                    p[d, t, h, rows, :] = new[d]
                if total is None or t == 0:
                    continue
                if k == 0:
                    for d in range(3):
                        gu[d, t - 1, h, pl.ds(rows.start - 8, 8), :] = g[d]
                    total = total + length
                else:
                    own = pl.ds(rows.start - 8, 8)
                    if k == 1:
                        s = [g[d] + gu[d, t - 1, h, own, :] for d in range(3)]
                        for d in range(3):
                            gu[d, t - 1, h, own, :] = s[d]
                    else:
                        s = [g[d] + 0.5 * gu[d, t - 1, h, own, :] for d in range(3)]
                    square = s[0] * s[0] + s[1] * s[1] + s[2] * s[2]
                    total = total + square * lax.rsqrt(jnp.maximum(square, TINY))
        return total

    def dual_range(k, c, g0, g1, total):
        def body(g, total):
            rows = rows_of(g)
            nexts, frame_nexts = cn[k, c], tcn[k, c]

            def ghost_of(t):
                if t == 0:
                    return pltpu.roll(frame_nexts, 127 - packed_at(4, g), 1)
                return pltpu.roll(nexts, 127 - packed_at(t, g), 1)

            return dual_group(k, rows, pl.ds(rows.start + 1, 8), range(5), ghost_of, total)

        return lax.fori_loop(g0, g1, body, total)

    def dual_above(k):
        @pl.when(jnp.logical_not(first_row))
        def _():
            nexts = rcn[k]
            dual_group(
                k, pl.ds(0, 8), pl.ds(1, 8), range(1, 5),
                lambda t: pltpu.roll(nexts, 127 - packed_at(t, 15), 1), None,
            )

    def dual_left(k, c):
        here, below_left, later_left = cp[k, c], rcp[k], tcp[k, c]
        later = jnp.where(lane >= 48, pltpu.roll(later_left, 48, 1), pltpu.roll(here, 112, 1))
        later = jnp.where(jnp.logical_and(lane >= 48, last_tm), here, later)
        last_group = jnp.bitwise_and(lane, 15) == 15
        follow = jnp.where(last_group, pltpu.roll(below_left, 15, 1), pltpu.roll(here, 127, 1))
        below = jnp.where(sublane == 7, pltpu.roll(follow, 7, 0), pltpu.roll(here, 7, 0))
        bottom = jnp.logical_and(jnp.logical_and(sublane == 7, last_group), last_row)
        below = jnp.where(bottom, here, below)
        g = [later - here, below - here, c0[k, c] - here]
        m = None if k == 0 else [pc[k, d] + SIGMA * g[d] for d in range(3)]
        new, _ = project(k, m, g)
        for d in range(3):
            pc[k + 1, d] = new[d]
        pc[k + 1, 3] = jnp.where(first_col, 0.0, new[2])

    def primal_range(k, g0, g1, carry):
        def body(g, carry):
            total, held = carry
            rows = rows_of(g)
            own = pl.ds(rows.start - 8, 8)
            before_rows = pl.ds(rows.start - 1, 8)
            left = pc[k + 1, 3]
            for t in range(1, 5):
                q = [p[2, t, h, rows, :] for h in range(2)]
                rolled = [pltpu.roll(q[h], 1, 1) for h in range(2)]
                ghost = pltpu.roll(left, 128 - packed_at(t, g), 1)
                before = [jnp.where(first_lane, ghost, rolled[0]), jnp.where(first_lane, rolled[0], rolled[1])]
                bars = []
                for h in range(2):
                    e = (
                        (p[0, t, h, rows, :] - p[0, t - 1, h, rows, :])
                        + (p[1, t, h, rows, :] - p[1, t, h, before_rows, :])
                        + (q[h] - before[h])
                    )
                    f = ub[0, t, h, rows, :]
                    scale = damp[t - 1, h, own, :]
                    total = total + (e * e * inv_fid[t - 1, h, own, :] + f * e)
                    if k == 0:
                        new = scale * (TAU * e)
                        bar = f + 2.0 * new
                    else:
                        old = res[t - 1, h, own, :]
                        total = total + old * old * fid[t - 1, h, own, :]
                        new = scale * (old + TAU * e)
                        bar = f + (2.0 * new - old)
                    if k < ITERS - 1:
                        res[t - 1, h, own, :] = new
                        ub[k + 1, t, h, rows, :] = bar
                        bars.append(bar)
                    else:
                        out_v[t - 1, h, own, :] = f + new
                if k < ITERS - 1:
                    held = packed(bars[0], bars[1], t, g, held)
            return total, held

        return lax.fori_loop(g0, g1, body, carry)

    def weights():
        for h in range(2):
            loads[2 * h + 1].wait()

        @pl.loop(0, GROUPS)
        def _(g):
            own = pl.ds(pl.multiple_of(8 * g, 8), 8)
            for t in range(4):
                for h in range(2):
                    lam = fid[t, h, own, :]
                    damp[t, h, own, :] = 1.0 / (1.0 + TAU * lam)
                    inv_fid[t, h, own, :] = 0.5 / lam
                    fid[t, h, own, :] = 0.5 * lam

    def send(k, c, held):
        c0[k, c], c255[k, c] = held
        start(frame_copies(k, c) + col_copies(k, c))
        if c == len(CHUNKS[k]) - 1:
            start(row_copies(k) + corner_copies(k))

    for h in range(2):
        loads[2 * h].wait()
    held = pack_first()
    pl.semaphore_wait(barrier, arrivals)
    for c in range(len(CHUNKS[0])):
        send(0, c, held)
    weights()

    sums = []
    for k in range(ITERS):
        length, total, held = zero, zero, (zero, zero)
        for c in range(len(CHUNKS[k])):
            if c == 0:
                wait_received(row_copies(k) + corner_copies(k))
            wait_received(frame_copies(k, c) + col_copies(k, c))

            @pl.when(last_tm)
            def _():
                ub[k, 5] = ub[k, 4]

            @pl.when(last_row)
            def _():
                for t in range(5):
                    for h in range(2):
                        ub[k, t, h, 136:137, :] = ub[k, t, h, 135:136, :]

            dual_left(k, c)
            if c == 0:
                dual_above(k)
            length = dual_range(k, c, *DUAL_STEPS[k][c], length)

            @pl.when(first_tm)
            def _():
                p[0, 0] = jnp.zeros_like(p[0, 0])

            for span in PRIMAL_STEPS[k][c]:
                total, held = primal_range(k, *span, (total, held))
            if k < ITERS - 1:
                send(k + 1, c, held)
        sums.append(total + (1.0 if k == 0 else 0.5) * length)

    puts = [
        pltpu.make_async_copy(out_v.at[:, h], out_hbm.at[:, :, pl.ds(128 * h, 128)], out_sem.at[h]) for h in range(2)
    ]
    for put in puts:
        put.start()

    row = jnp.zeros((1, 128), F32)
    row_lane = lax.broadcasted_iota(jnp.int32, (1, 128), 1)
    for k in range(ITERS):
        row = jnp.where(row_lane == k, jnp.sum(sums[k]), row)

    def exchange(mine, slots, me, count, mate, i, row):
        mine[0] = row
        slots[me] = row

        @pl.loop(1, count)
        def _(j):
            pltpu.make_async_remote_copy(
                src_ref=mine.at[0], dst_ref=slots.at[me], send_sem=ar_send.at[i], recv_sem=ar_recv.at[i],
                device_id=mate(j), device_id_type=MESH,
            ).start()

        landed = slots.at[pl.ds(0, count - 1)]
        pltpu.make_async_copy(landed, landed, ar_recv.at[i]).wait()
        got = slots[0]
        for j in range(1, count):
            got = got + slots[j]
        return got

    def drain(slots, count, i):
        landed = slots.at[pl.ds(0, count - 1)]
        pltpu.make_async_copy(landed, landed, ar_send.at[i]).wait()

    row = exchange(part, plane, at[0] * n_col + at[2], n_tm * n_col, plane_mate, 0, row)
    row = exchange(part2, line, at[1], n_row, line_mate, 1, row)
    cells = float(4 * 128 * 256) * float(n_tm * n_row * n_col)
    gaps_ref[...] = row * (1.0 / cells)

    for k in range(ITERS):
        wait_sent(all_copies(k))
    drain(plane, n_tm * n_col, 0)
    drain(line, n_row, 1)
    for put in puts:
        put.wait()


def on_device(sizes, noisy_video, fidelity):
    n_chunks = max(len(c) for c in CHUNKS)
    dma = pltpu.SemaphoreType.DMA
    vmem = lambda *shape: pltpu.VMEM(shape, F32)
    n_plane, n_row = sizes[0] * sizes[2], sizes[1]
    out, gaps = pl.pallas_call(
        functools.partial(kernel, sizes),
        out_shape=(jax.ShapeDtypeStruct(noisy_video.shape, F32), jax.ShapeDtypeStruct((1, 128), F32)),
        in_specs=[pl.BlockSpec(memory_space=pl.ANY)] * 2,
        out_specs=(pl.BlockSpec(memory_space=pl.ANY), pl.BlockSpec(memory_space=pltpu.VMEM)),
        scratch_shapes=[
            vmem(3, 6, 2, 144, 128),
            vmem(3, 5, 2, 136, 128),
            vmem(3, 4, 2, 128, 128),
            vmem(4, 2, 128, 128),
            vmem(4, 2, 128, 128),
            vmem(4, 2, 128, 128),
            vmem(4, 2, 128, 128),
            vmem(4, 2, 128, 128),
            vmem(3, n_chunks, 8, 128),
            vmem(3, n_chunks, 8, 128),
            vmem(3, n_chunks, 8, 128),
            vmem(3, n_chunks, 8, 128),
            vmem(3, n_chunks, 8, 128),
            vmem(3, n_chunks, 8, 128),
            vmem(3, 8, 128),
            vmem(3, 8, 128),
            vmem(4, 4, 8, 128),
            vmem(1, 1, 128),
            vmem(n_plane, 1, 128),
            vmem(1, 1, 128),
            vmem(n_row, 1, 128),
            dma((4,)),
            dma((2,)),
            dma((3, n_chunks, 2)), dma((3, n_chunks, 2)),
            dma((3, 2)), dma((3, 2)),
            dma((3, n_chunks, 2)), dma((3, n_chunks, 2)),
            dma((3, 2)), dma((3, 2)),
            dma((3, n_chunks, 2)), dma((3, n_chunks, 2)),
            dma((3, 2)), dma((3, 2)),
            dma((2,)), dma((2,)),
        ],
        compiler_params=pltpu.CompilerParams(collective_id=0, has_side_effects=True),
    )(noisy_video, fidelity)
    return out, gaps[0, :3]


def solution(mesh):
    sizes = (mesh.shape["tm"], mesh.shape["row"], mesh.shape["col"])
    placed = P("tm", "row", "col")
    return jax.shard_map(
        functools.partial(on_device, sizes),
        mesh=mesh,
        in_specs=(placed, placed),
        out_specs=(placed, P()),
        check_vma=False,
    )
```

```python
import functools
from itertools import zip_longest

import jax
import jax.numpy as jnp
from jax import lax
from jax.experimental import pallas as pl
from jax.experimental.pallas import tpu as pltpu
from jax.sharding import PartitionSpec as P

ITERS = 3
SIGMA = 0.28
TAU = 0.28
TINY = 1.1754943508222875e-38
MESH = pl.DeviceIdType.MESH
F32 = jnp.float32

GROUPS = 16

FRAME_UP, FRAME_DOWN = (1, 0, 0), (-1, 0, 0)
ROW_UP, ROW_DOWN = (0, 1, 0), (0, -1, 0)
COL_UP, COL_DOWN = (0, 0, 1), (0, 0, -1)
NEIGHBOURS = (
    FRAME_UP, FRAME_DOWN, ROW_UP, ROW_DOWN, COL_UP, COL_DOWN,
    (1, -1, 0), (-1, 1, 0), (1, 0, -1), (-1, 0, 1), (0, 1, -1), (0, -1, 1),
)

CHUNKS = ([(0, 16)], [(0, 16)], [(0, 16)])
DUAL_STEPS = ([(0, 16)], [(0, 16)], [(0, 16)])
PRIMAL_STEPS = ([[(0, 16)]], [[(0, 16)]], [[(0, 16)]])


UNROLL = 4
PACK_UNROLL = 8


def grouped(g0, g1, body, carry, unroll):
    steps = (g1 - g0) // unroll

    def step(i, carry):
        for u in range(unroll):
            carry = body(g0 + i * unroll + u, carry)
        return carry

    if steps > 1:
        carry = lax.fori_loop(0, steps, step, carry)
    elif steps == 1:
        carry = step(0, carry)
    for g in range(g0 + steps * unroll, g1):
        carry = body(g, carry)
    return carry


def rows_of(group):
    start = 8 + 8 * group
    return pl.ds(start if isinstance(start, int) else pl.multiple_of(start, 8), 8)


def kernel(
    sizes, f_hbm, fid_hbm, out_hbm, gaps_ref,
    ub, p, gu, res, damp, inv_fid, fid, out_v, c0, c255, cn, cp, tcn, tcp, rcn, rcp, pc, part, by_col, by_tm, by_row,
    load_sem, out_sem,
    fr_send, fr_recv, row_send, row_recv, col_send, col_recv, tr_send, tr_recv, tc_send, tc_recv, rc_send, rc_recv,
    ar_send, ar_recv, token_sem,
):
    n_tm, n_row, n_col = sizes
    at = (lax.axis_index("tm"), lax.axis_index("row"), lax.axis_index("col"))

    def there(step):
        return dict(tm=at[0] + step[0], row=at[1] + step[1], col=at[2] + step[2])

    def exists(step):
        found = None
        for pos, size, move in zip(at, sizes, step):
            if move:
                ok = pos < size - 1 if move > 0 else pos > 0
                found = ok if found is None else jnp.logical_and(found, ok)
        return found

    lane = lax.broadcasted_iota(jnp.int32, (8, 128), 1)
    sublane = lax.broadcasted_iota(jnp.int32, (8, 128), 0)
    first_lane, last_lane = lane == 0, lane == 127
    first_row, first_col, first_tm = at[1] == 0, at[2] == 0, at[0] == 0
    last_row, last_col, last_tm = at[1] == n_row - 1, at[2] == n_col - 1, at[0] == n_tm - 1
    edge_lane = jnp.logical_and(last_lane, last_col)

    loads = []
    for h in range(2):
        cols = pl.ds(128 * h, 128)
        loads.append(pltpu.make_async_copy(f_hbm.at[:, :, cols], ub.at[0, 1:5, h, 8:136, :], load_sem.at[h]))
        loads.append(pltpu.make_async_copy(fid_hbm.at[:, :, cols], fid.at[:, h], load_sem.at[2 + h]))
    for load in (loads[0], loads[2], loads[1], loads[3]):
        load.start()

    def ring(**moves):
        out = {}
        for name, pos, size in zip(("tm", "row", "col"), at, sizes):
            out[name] = lax.rem(pos + (moves.get(name, 0) + size), size)
        return out

    barrier = pltpu.get_barrier_semaphore()
    arrivals = 0
    for move in NEIGHBOURS:
        if sum(map(abs, move)) == 1:
            pl.semaphore_signal(
                barrier, inc=1, device_id=ring(tm=move[0], row=move[1], col=move[2]), device_id_type=MESH)
            arrivals = arrivals + 1
            continue
        ok = exists(move)

        @pl.when(ok)
        def _():
            pl.semaphore_signal(barrier, inc=1, device_id=there(move), device_id_type=MESH)

        arrivals = arrivals + ok.astype(jnp.int32)

    def tokens(name, count):
        reach, out = 1, []
        while 2 * reach < count:
            out.append((name, reach))
            reach *= 2
        return out

    rounds = list(zip_longest(tokens("row", n_row), tokens("col", n_col), tokens("tm", n_tm)))

    def tell(i):
        for j, token in enumerate(rounds[i] if i < len(rounds) else ()):
            if token:
                name, reach = token
                for d in (reach, -reach):
                    pl.semaphore_signal(
                        token_sem.at[i, j], inc=1, device_id=ring(**{name: d}), device_id_type=MESH)

    def hear(i):
        for j, token in enumerate(rounds[i] if i < len(rounds) else ()):
            if token:
                pl.semaphore_wait(token_sem.at[i, j], 2)

    zero = jnp.zeros((8, 128), F32)
    p[...] = jnp.zeros_like(p)

    def remote(src, dst, send, recv, step):
        return pltpu.make_async_remote_copy(
            src_ref=src, dst_ref=dst, send_sem=send, recv_sem=recv, device_id=there(step), device_id_type=MESH
        )

    def frame_copies(k, c):
        g0, g1 = CHUNKS[k][c]
        out = []
        rows = pl.ds(8 + 8 * g0, 8 * (g1 - g0))
        for i, (step, src, dst) in enumerate(((FRAME_DOWN, 1, 5), (FRAME_UP, 4, 0))):
            out.append((step, remote(
                ub.at[k, src, :, rows, :], ub.at[k, dst, :, rows, :], fr_send.at[k, c, i], fr_recv.at[k, c, i], step)))
        return out

    def row_copies(k):
        out = []
        low, high = pl.ds(8, 8), pl.ds(128, 8)
        ghost_low, ghost_high = pl.ds(0, 8), pl.ds(136, 8)
        for i, (step, src, dst) in enumerate(((ROW_DOWN, low, ghost_high), (ROW_UP, high, ghost_low))):
            out.append((step, remote(
                ub.at[k, 1:5, :, src, :], ub.at[k, 1:5, :, dst, :], row_send.at[k, i], row_recv.at[k, i], step)))
        out.append(((1, -1, 0), remote(
            ub.at[k, 4, :, low, :], ub.at[k, 0, :, ghost_high, :], tr_send.at[k, 0], tr_recv.at[k, 0], (1, -1, 0))))
        out.append(((-1, 1, 0), remote(
            ub.at[k, 1, :, high, :], ub.at[k, 5, :, ghost_low, :], tr_send.at[k, 1], tr_recv.at[k, 1], (-1, 1, 0))))
        return out

    def col_copies(k, c):
        return [
            (COL_DOWN, remote(c0.at[k, c], cn.at[k, c], col_send.at[k, c, 0], col_recv.at[k, c, 0], COL_DOWN)),
            (COL_UP, remote(c255.at[k, c], cp.at[k, c], col_send.at[k, c, 1], col_recv.at[k, c, 1], COL_UP)),
            ((1, 0, -1), remote(c0.at[k, c], tcn.at[k, c], tc_send.at[k, c, 0], tc_recv.at[k, c, 0], (1, 0, -1))),
            ((-1, 0, 1), remote(c255.at[k, c], tcp.at[k, c], tc_send.at[k, c, 1], tc_recv.at[k, c, 1], (-1, 0, 1))),
        ]

    def corner_copies(k):
        c = len(CHUNKS[k]) - 1
        return [
            ((0, 1, -1), remote(c0.at[k, c], rcn.at[k], rc_send.at[k, 0], rc_recv.at[k, 0], (0, 1, -1))),
            ((0, -1, 1), remote(c255.at[k, c], rcp.at[k], rc_send.at[k, 1], rc_recv.at[k, 1], (0, -1, 1))),
        ]

    def start(copies):
        for step, copy in copies:
            @pl.when(exists(step))
            def _():
                copy.start()

    def wait_sent(copies):
        for step, copy in copies:
            @pl.when(exists(step))
            def _():
                copy.wait_send()

    def wait_received(copies):
        for step, copy in copies:
            @pl.when(exists(tuple(-s for s in step)))
            def _():
                copy.wait_recv()

    def all_copies(k):
        out = row_copies(k) + corner_copies(k)
        for c in range(len(CHUNKS[k])):
            out += frame_copies(k, c) + col_copies(k, c)
        return out

    def packed_at(t, g):
        return (t - 1) * 16 + g

    def packed(x0, x1, t, g, held):
        i = packed_at(t, g)
        here = lane == i
        return (
            jnp.where(here, pltpu.roll(x0, i, 1), held[0]),
            jnp.where(here, pltpu.roll(x1, i + 1, 1), held[1]),
        )

    def pack(k, g0, g1, held):
        def body(g, held):
            for t in range(1, 5):
                held = packed(ub[k, t, 0, rows_of(g), :], ub[k, t, 1, rows_of(g), :], t, g, held)
            return held

        return grouped(g0, g1, body, held, PACK_UNROLL)

    def project(k, m, g):
        if k == 0:
            square = g[0] * g[0] + g[1] * g[1] + g[2] * g[2]
            root = lax.rsqrt(jnp.maximum(square, TINY))
            scale = jnp.minimum(SIGMA, root)
            return [g[d] * scale for d in range(3)], square * root
        square = m[0] * m[0] + m[1] * m[1] + m[2] * m[2]
        scale = lax.rsqrt(jnp.maximum(square, 1.0))
        return [m[d] * scale for d in range(3)], None

    def dual_group(k, rows, below, frames, ghost_of, total):
        x = [[ub[k, t, h, rows, :] for h in range(2)] for t in range(frames[0], 6)]
        for t in frames:
            here, later = x[t - frames[0]], x[t - frames[0] + 1]
            rolled = [pltpu.roll(here[h], 127, 1) for h in range(2)]
            after = [
                jnp.where(last_lane, rolled[1], rolled[0]),
                jnp.where(edge_lane, here[1], jnp.where(last_lane, ghost_of(t), rolled[1])),
            ]
            for h in range(2):
                g = [later[h] - here[h], ub[k, t, h, below, :] - here[h], after[h] - here[h]]
                m = None if k == 0 else [p[d, t, h, rows, :] + SIGMA * g[d] for d in range(3)]
                new, length = project(k, m, g)
                for d in range(3):
                    p[d, t, h, rows, :] = new[d]
                if total is None or t == 0:
                    continue
                if k == 0:
                    for d in range(3):
                        gu[d, t - 1, h, pl.ds(rows.start - 8, 8), :] = g[d]
                    total = total + length
                else:
                    own = pl.ds(rows.start - 8, 8)
                    if k == 1:
                        s = [g[d] + gu[d, t - 1, h, own, :] for d in range(3)]
                        for d in range(3):
                            gu[d, t - 1, h, own, :] = s[d]
                    else:
                        s = [g[d] + 0.5 * gu[d, t - 1, h, own, :] for d in range(3)]
                    square = s[0] * s[0] + s[1] * s[1] + s[2] * s[2]
                    total = total + square * lax.rsqrt(jnp.maximum(square, TINY))
        return total

    def dual_range(k, c, g0, g1, total):
        def body(g, total):
            rows = rows_of(g)
            nexts, frame_nexts = cn[k, c], tcn[k, c]

            def ghost_of(t):
                if t == 0:
                    return pltpu.roll(frame_nexts, 127 - packed_at(4, g), 1)
                return pltpu.roll(nexts, 127 - packed_at(t, g), 1)

            return dual_group(k, rows, pl.ds(rows.start + 1, 8), range(5), ghost_of, total)

        return grouped(g0, g1, body, total, UNROLL)

    def dual_above(k):
        @pl.when(jnp.logical_not(first_row))
        def _():
            nexts = rcn[k]
            dual_group(
                k, pl.ds(0, 8), pl.ds(1, 8), range(1, 5),
                lambda t: pltpu.roll(nexts, 127 - packed_at(t, 15), 1), None,
            )

    def dual_left(k, c):
        here, below_left, later_left = cp[k, c], rcp[k], tcp[k, c]
        later = jnp.where(lane >= 48, pltpu.roll(later_left, 48, 1), pltpu.roll(here, 112, 1))
        later = jnp.where(jnp.logical_and(lane >= 48, last_tm), here, later)
        last_group = jnp.bitwise_and(lane, 15) == 15
        follow = jnp.where(last_group, pltpu.roll(below_left, 15, 1), pltpu.roll(here, 127, 1))
        below = jnp.where(sublane == 7, pltpu.roll(follow, 7, 0), pltpu.roll(here, 7, 0))
        bottom = jnp.logical_and(jnp.logical_and(sublane == 7, last_group), last_row)
        below = jnp.where(bottom, here, below)
        g = [later - here, below - here, c0[k, c] - here]
        m = None if k == 0 else [pc[k, d] + SIGMA * g[d] for d in range(3)]
        new, _ = project(k, m, g)
        for d in range(3):
            pc[k + 1, d] = new[d]
        pc[k + 1, 3] = jnp.where(first_col, 0.0, new[2])

    def primal_range(k, g0, g1, total):
        def body(g, total):
            rows = rows_of(g)
            own = pl.ds(rows.start - 8, 8)
            before_rows = pl.ds(rows.start - 1, 8)
            left = pc[k + 1, 3]
            for t in range(1, 5):
                q = [p[2, t, h, rows, :] for h in range(2)]
                rolled = [pltpu.roll(q[h], 1, 1) for h in range(2)]
                ghost = pltpu.roll(left, 128 - packed_at(t, g), 1)
                before = [jnp.where(first_lane, ghost, rolled[0]), jnp.where(first_lane, rolled[0], rolled[1])]
                for h in range(2):
                    e = (
                        (p[0, t, h, rows, :] - p[0, t - 1, h, rows, :])
                        + (p[1, t, h, rows, :] - p[1, t, h, before_rows, :])
                        + (q[h] - before[h])
                    )
                    f = ub[0, t, h, rows, :]
                    scale = damp[t - 1, h, own, :]
                    total = total + (e * e * inv_fid[t - 1, h, own, :] + f * e)
                    if k == 0:
                        new = scale * (TAU * e)
                        bar = f + 2.0 * new
                    else:
                        old = res[t - 1, h, own, :]
                        total = total + old * old * fid[t - 1, h, own, :]
                        new = scale * (old + TAU * e)
                        bar = f + (2.0 * new - old)
                    if k < ITERS - 1:
                        res[t - 1, h, own, :] = new
                        ub[k + 1, t, h, rows, :] = bar
                    else:
                        out_v[t - 1, h, own, :] = f + new
            return total

        return grouped(g0, g1, body, total, UNROLL)

    def weights():
        for h in range(2):
            loads[2 * h + 1].wait()

        @pl.loop(0, GROUPS)
        def _(g):
            own = pl.ds(pl.multiple_of(8 * g, 8), 8)
            for t in range(4):
                for h in range(2):
                    lam = fid[t, h, own, :]
                    damp[t, h, own, :] = 1.0 / (1.0 + TAU * lam)
                    inv_fid[t, h, own, :] = 0.5 / lam
                    fid[t, h, own, :] = 0.5 * lam

    def send(k, c, held):
        c0[k, c], c255[k, c] = held
        start(frame_copies(k, c) + col_copies(k, c))
        if c == len(CHUNKS[k]) - 1:
            start(row_copies(k) + corner_copies(k))

    for h in range(2):
        loads[2 * h].wait()
    held = pack(0, 0, GROUPS, (zero, zero))
    pl.semaphore_wait(barrier, arrivals)
    tell(0)
    for c in range(len(CHUNKS[0])):
        send(0, c, held)
    weights()

    hear(0)
    tell(1)

    sums = []
    for k in range(ITERS):
        length, total, held = zero, zero, (zero, zero)
        for c in range(len(CHUNKS[k])):
            if c == 0:
                wait_received(row_copies(k) + corner_copies(k))
            wait_received(frame_copies(k, c) + col_copies(k, c))

            @pl.when(last_tm)
            def _():
                ub[k, 5] = ub[k, 4]

            @pl.when(last_row)
            def _():
                for t in range(5):
                    for h in range(2):
                        ub[k, t, h, 136:137, :] = ub[k, t, h, 135:136, :]

            if c == 0:
                hear(k + 1)
                tell(k + 2)
            dual_left(k, c)
            if c == 0:
                dual_above(k)
            length = dual_range(k, c, *DUAL_STEPS[k][c], length)

            @pl.when(first_tm)
            def _():
                p[0, 0] = jnp.zeros_like(p[0, 0])

            for span in PRIMAL_STEPS[k][c]:
                total = primal_range(k, *span, total)
                if k < ITERS - 1:
                    held = pack(k + 1, *span, held)
            if k < ITERS - 1:
                send(k + 1, c, held)
        sums.append(total + (1.0 if k == 0 else 0.5) * length)

    puts = [
        pltpu.make_async_copy(out_v.at[:, h], out_hbm.at[:, :, pl.ds(128 * h, 128)], out_sem.at[h]) for h in range(2)
    ]
    for put in puts:
        put.start()

    row = jnp.zeros((1, 128), F32)
    row_lane = lax.broadcasted_iota(jnp.int32, (1, 128), 1)
    for k in range(ITERS):
        row = jnp.where(row_lane == k, jnp.sum(sums[k]), row)

    def exchange(mine, slots, me, count, name, i, row):
        mine[...] = row
        slots[me] = row

        @pl.loop(1, count)
        def _(j):
            pltpu.make_async_remote_copy(
                src_ref=mine, dst_ref=slots.at[me], send_sem=ar_send.at[i], recv_sem=ar_recv.at[i],
                device_id=ring(**{name: j}), device_id_type=MESH,
            ).start()

        landed = slots.at[pl.ds(0, count - 1)]
        pltpu.make_async_copy(landed, landed, ar_recv.at[i]).wait()
        got = slots[0]
        for j in range(1, count):
            got = got + slots[j]
        return got

    def drain(slots, count, i):
        landed = slots.at[pl.ds(0, count - 1)]
        pltpu.make_async_copy(landed, landed, ar_send.at[i]).wait()

    row = exchange(part.at[0], by_col, at[2], n_col, "col", 0, row)
    row = exchange(part.at[1], by_tm, at[0], n_tm, "tm", 1, row)
    row = exchange(part.at[2], by_row, at[1], n_row, "row", 2, row)
    cells = float(4 * 128 * 256) * float(n_tm * n_row * n_col)
    gaps_ref[...] = row * (1.0 / cells)

    for k in range(ITERS):
        wait_sent(all_copies(k))
    drain(by_col, n_col, 0)
    drain(by_tm, n_tm, 1)
    drain(by_row, n_row, 2)
    for put in puts:
        put.wait()


def on_device(sizes, noisy_video, fidelity):
    n_chunks = max(len(c) for c in CHUNKS)
    dma = pltpu.SemaphoreType.DMA
    vmem = lambda *shape: pltpu.VMEM(shape, F32)
    out, gaps = pl.pallas_call(
        functools.partial(kernel, sizes),
        out_shape=(jax.ShapeDtypeStruct(noisy_video.shape, F32), jax.ShapeDtypeStruct((1, 128), F32)),
        in_specs=[pl.BlockSpec(memory_space=pl.ANY)] * 2,
        out_specs=(pl.BlockSpec(memory_space=pl.ANY), pl.BlockSpec(memory_space=pltpu.VMEM)),
        scratch_shapes=[
            vmem(3, 6, 2, 144, 128),
            vmem(3, 5, 2, 136, 128),
            vmem(3, 4, 2, 128, 128),
            vmem(4, 2, 128, 128),
            vmem(4, 2, 128, 128),
            vmem(4, 2, 128, 128),
            vmem(4, 2, 128, 128),
            vmem(4, 2, 128, 128),
            vmem(3, n_chunks, 8, 128),
            vmem(3, n_chunks, 8, 128),
            vmem(3, n_chunks, 8, 128),
            vmem(3, n_chunks, 8, 128),
            vmem(3, n_chunks, 8, 128),
            vmem(3, n_chunks, 8, 128),
            vmem(3, 8, 128),
            vmem(3, 8, 128),
            vmem(4, 4, 8, 128),
            vmem(3, 1, 128),
            vmem(sizes[2], 1, 128),
            vmem(sizes[0], 1, 128),
            vmem(sizes[1], 1, 128),
            dma((4,)),
            dma((2,)),
            dma((3, n_chunks, 2)), dma((3, n_chunks, 2)),
            dma((3, 2)), dma((3, 2)),
            dma((3, n_chunks, 2)), dma((3, n_chunks, 2)),
            dma((3, 2)), dma((3, 2)),
            dma((3, n_chunks, 2)), dma((3, n_chunks, 2)),
            dma((3, 2)), dma((3, 2)),
            dma((3,)), dma((3,)),
            pltpu.SemaphoreType.REGULAR((4, 3)),
        ],
        compiler_params=pltpu.CompilerParams(collective_id=0, has_side_effects=True),
    )(noisy_video, fidelity)
    return out, gaps[0, :3]


def solution(mesh):
    sizes = (mesh.shape["tm"], mesh.shape["row"], mesh.shape["col"])
    placed = P("tm", "row", "col")
    return jax.shard_map(
        functools.partial(on_device, sizes),
        mesh=mesh,
        in_specs=(placed, placed),
        out_specs=(placed, P()),
        check_vma=False,
    )
```

```python
import functools
from itertools import zip_longest

import jax
import jax.numpy as jnp
from jax import lax
from jax.experimental import pallas as pl
from jax.experimental.pallas import tpu as pltpu
from jax.sharding import PartitionSpec as P

ITERS = 3
SIGMA = 0.28
TAU = 0.28
TINY = 1.1754943508222875e-38
MESH = pl.DeviceIdType.MESH
F32 = jnp.float32

GROUPS = 16

FRAME_UP, FRAME_DOWN = (1, 0, 0), (-1, 0, 0)
ROW_UP, ROW_DOWN = (0, 1, 0), (0, -1, 0)
COL_UP, COL_DOWN = (0, 0, 1), (0, 0, -1)
NEIGHBOURS = (
    FRAME_UP, FRAME_DOWN, ROW_UP, ROW_DOWN, COL_UP, COL_DOWN,
    (1, -1, 0), (-1, 1, 0), (1, 0, -1), (-1, 0, 1), (0, 1, -1), (0, -1, 1),
)

CHUNKS = (
    ([(0, 5)], [(5, 9)], [(9, 13)], [(13, 16)]),
    ([(0, 4)], [(4, 8)], [(8, 12)], [(12, 16)]),
    ([(1, 3)], [(3, 7)], [(7, 11)], [(11, 16), (0, 1)]),
)
DUAL_STEPS = (
    ([(0, 4)], [(4, 8)], [(8, 12)], [(12, 16)]),
    ([(0, 3)], [(3, 7)], [(7, 11)], [(11, 16)]),
    ([(1, 2)], [(2, 6)], [(6, 10)], [(10, 16), (0, 1)]),
)
PRIMAL_STEPS = (
    ([(0, 4)], [(4, 8)], [(8, 12)], [(12, 16)]),
    ([(1, 3)], [(3, 7)], [(7, 11)], [(11, 16), (0, 1)]),
    ([], [(2, 6)], [(6, 10)], [(10, 16), (0, 2)]),
)
STEPS = 4
ABOVE_STEP = (0, 3, 3)
LOW_CHUNK = (3, 0, 3)

UNROLL = 4
PACK_UNROLL = 5


def grouped(g0, g1, body, carry, unroll):
    steps = (g1 - g0) // unroll

    def step(i, carry):
        for u in range(unroll):
            carry = body(g0 + i * unroll + u, carry)
        return carry

    if steps > 1:
        carry = lax.fori_loop(0, steps, step, carry)
    elif steps == 1:
        carry = step(0, carry)
    for g in range(g0 + steps * unroll, g1):
        carry = body(g, carry)
    return carry


def rows_of(group):
    start = 8 + 8 * group
    return pl.ds(start if isinstance(start, int) else pl.multiple_of(start, 8), 8)


def kernel(
    sizes, f_hbm, fid_hbm, out_v, gaps_ref,
    ub, p, gu, res, damp, inv_fid, fid, c0, c255, cn, cp, tcn, tcp, rcn, rcp, pc, part, by_col, by_tm, by_row,
    load_sem,
    fr_send, fr_recv, row_send, row_recv, col_send, col_recv, tr_send, tr_recv, tc_send, tc_recv, rc_send, rc_recv,
    ar_send, ar_recv, token_sem,
):
    n_tm, n_row, n_col = sizes
    at = (lax.axis_index("tm"), lax.axis_index("row"), lax.axis_index("col"))

    def there(step):
        return dict(tm=at[0] + step[0], row=at[1] + step[1], col=at[2] + step[2])

    def exists(step):
        found = None
        for pos, size, move in zip(at, sizes, step):
            if move:
                ok = pos < size - 1 if move > 0 else pos > 0
                found = ok if found is None else jnp.logical_and(found, ok)
        return found

    lane = lax.broadcasted_iota(jnp.int32, (8, 128), 1)
    sublane = lax.broadcasted_iota(jnp.int32, (8, 128), 0)
    first_lane, last_lane = lane == 0, lane == 127
    first_row, first_col, first_tm = at[1] == 0, at[2] == 0, at[0] == 0
    last_row, last_col, last_tm = at[1] == n_row - 1, at[2] == n_col - 1, at[0] == n_tm - 1
    edge_lane = jnp.logical_and(last_lane, last_col)

    frame_loads, fid_loads = {}, []
    for h in range(2):
        cols = pl.ds(128 * h, 128)
        for t in range(4):
            frame_loads[t, h] = pltpu.make_async_copy(
                f_hbm.at[t, :, cols], ub.at[0, t + 1, h, 8:136, :], load_sem.at[t, h])
        fid_loads.append(pltpu.make_async_copy(fid_hbm.at[:, :, cols], fid.at[:, h], load_sem.at[4, h]))
    for t in (0, 3, 1, 2):
        for h in range(2):
            frame_loads[t, h].start()
    for load in fid_loads:
        load.start()

    def ring(**moves):
        out = {}
        for name, pos, size in zip(("tm", "row", "col"), at, sizes):
            out[name] = lax.rem(pos + (moves.get(name, 0) + size), size)
        return out

    barrier = pltpu.get_barrier_semaphore()
    arrivals = 0
    for move in NEIGHBOURS:
        if sum(map(abs, move)) == 1:
            pl.semaphore_signal(
                barrier, inc=1, device_id=ring(tm=move[0], row=move[1], col=move[2]), device_id_type=MESH)
            arrivals = arrivals + 1
            continue
        ok = exists(move)

        @pl.when(ok)
        def _():
            pl.semaphore_signal(barrier, inc=1, device_id=there(move), device_id_type=MESH)

        arrivals = arrivals + ok.astype(jnp.int32)

    def tokens(name, count):
        reach, out = 1, []
        while 2 * reach < count:
            out.append((name, reach))
            reach *= 2
        return out

    rounds = list(zip_longest(tokens("row", n_row), tokens("col", n_col), tokens("tm", n_tm)))

    def tell(i):
        for j, token in enumerate(rounds[i] if i < len(rounds) else ()):
            if token:
                name, reach = token
                for d in (reach, -reach):
                    pl.semaphore_signal(
                        token_sem.at[i, j], inc=1, device_id=ring(**{name: d}), device_id_type=MESH)

    def hear(i):
        for j, token in enumerate(rounds[i] if i < len(rounds) else ()):
            if token:
                pl.semaphore_wait(token_sem.at[i, j], 2)

    zero = jnp.zeros((8, 128), F32)

    @pl.when(first_row)
    def _():
        for t in range(1, 5):
            for h in range(2):
                p[1, t, h, 0:8, :] = zero

    def remote(src, dst, send, recv, step):
        return pltpu.make_async_remote_copy(
            src_ref=src, dst_ref=dst, send_sem=send, recv_sem=recv, device_id=there(step), device_id_type=MESH
        )

    def frame_copies(k, c):
        out = []
        for i, (move, src, dst) in enumerate(((FRAME_DOWN, 1, 5), (FRAME_UP, 4, 0))):
            for j, (g0, g1) in enumerate(CHUNKS[k][c]):
                rows = pl.ds(8 + 8 * g0, 8 * (g1 - g0))
                out.append((move, remote(
                    ub.at[k, src, :, rows, :], ub.at[k, dst, :, rows, :],
                    fr_send.at[k, c, i, j], fr_recv.at[k, c, i, j], move)))
        return out

    low, high, ghost_low, ghost_high = pl.ds(8, 8), pl.ds(128, 8), pl.ds(0, 8), pl.ds(136, 8)

    def low_copies(k):
        c = LOW_CHUNK[k]
        return [
            (ROW_DOWN, remote(
                ub.at[k, 1:5, :, low, :], ub.at[k, 1:5, :, ghost_high, :], row_send.at[k, 0], row_recv.at[k, 0], ROW_DOWN)),
            ((1, -1, 0), remote(
                ub.at[k, 4, :, low, :], ub.at[k, 0, :, ghost_high, :], tr_send.at[k, 0], tr_recv.at[k, 0], (1, -1, 0))),
            ((0, -1, 1), remote(c255.at[k, c], rcp.at[k], rc_send.at[k, 1], rc_recv.at[k, 1], (0, -1, 1))),
        ]

    def high_copies(k):
        c = STEPS - 1
        return [
            (ROW_UP, remote(
                ub.at[k, 1:5, :, high, :], ub.at[k, 1:5, :, ghost_low, :], row_send.at[k, 1], row_recv.at[k, 1], ROW_UP)),
            ((-1, 1, 0), remote(
                ub.at[k, 1, :, high, :], ub.at[k, 5, :, ghost_low, :], tr_send.at[k, 1], tr_recv.at[k, 1], (-1, 1, 0))),
            ((0, 1, -1), remote(c0.at[k, c], rcn.at[k], rc_send.at[k, 0], rc_recv.at[k, 0], (0, 1, -1))),
        ]

    def col_copies(k, c):
        return [
            (COL_DOWN, remote(c0.at[k, c], cn.at[k, c], col_send.at[k, c, 0], col_recv.at[k, c, 0], COL_DOWN)),
            (COL_UP, remote(c255.at[k, c], cp.at[k, c], col_send.at[k, c, 1], col_recv.at[k, c, 1], COL_UP)),
            ((1, 0, -1), remote(c0.at[k, c], tcn.at[k, c], tc_send.at[k, c, 0], tc_recv.at[k, c, 0], (1, 0, -1))),
            ((-1, 0, 1), remote(c255.at[k, c], tcp.at[k, c], tc_send.at[k, c, 1], tc_recv.at[k, c, 1], (-1, 0, 1))),
        ]

    def start(copies):
        for step, copy in copies:
            @pl.when(exists(step))
            def _():
                copy.start()

    def wait_sent(copies):
        for step, copy in copies:
            @pl.when(exists(step))
            def _():
                copy.wait_send()

    def wait_received(copies):
        for step, copy in copies:
            @pl.when(exists(tuple(-s for s in step)))
            def _():
                copy.wait_recv()

    def col_chunks(k):
        return range(STEPS) if k else range(STEPS - 1, STEPS)

    def all_copies(k):
        out = low_copies(k) + high_copies(k)
        for c in range(STEPS):
            out += frame_copies(k, c)
        for c in col_chunks(k):
            out += col_copies(k, c)
        return out

    def packed_at(t, g):
        return (t - 1) * 16 + g

    def packed(x0, x1, t, g, held):
        i = packed_at(t, g)
        here = lane == i
        return (
            jnp.where(here, pltpu.roll(x0, i, 1), held[0]),
            jnp.where(here, pltpu.roll(x1, i + 1, 1), held[1]),
        )

    def pack(k, g0, g1, held):
        def body(g, held):
            for t in range(1, 5):
                held = packed(ub[k, t, 0, rows_of(g), :], ub[k, t, 1, rows_of(g), :], t, g, held)
            return held

        return grouped(g0, g1, body, held, PACK_UNROLL)

    def project(k, m, g):
        if k == 0:
            square = g[0] * g[0] + g[1] * g[1] + g[2] * g[2]
            root = lax.rsqrt(jnp.maximum(square, TINY))
            scale = jnp.minimum(SIGMA, root)
            return [g[d] * scale for d in range(3)], square * root
        square = m[0] * m[0] + m[1] * m[1] + m[2] * m[2]
        scale = lax.rsqrt(jnp.maximum(square, 1.0))
        return [m[d] * scale for d in range(3)], None

    def dual_group(k, rows, below, frames, ghost_of, total):
        x = [[ub[k, t, h, rows, :] for h in range(2)] for t in range(frames[0], 6)]
        for t in frames:
            here, later = x[t - frames[0]], x[t - frames[0] + 1]
            if t == 4:
                later = [jnp.where(last_tm, here[h], later[h]) for h in range(2)]
            rolled = [pltpu.roll(here[h], 127, 1) for h in range(2)]
            after = [
                jnp.where(last_lane, rolled[1], rolled[0]),
                jnp.where(edge_lane, here[1], jnp.where(last_lane, ghost_of(t), rolled[1])),
            ]
            for h in range(2):
                g = [later[h] - here[h], ub[k, t, h, below, :] - here[h], after[h] - here[h]]
                m = None if k == 0 else [p[d, t, h, rows, :] + SIGMA * g[d] for d in range(3)]
                new, length = project(k, m, g)
                if t == 0:
                    new[0] = jnp.where(first_tm, 0.0, new[0])
                for d in range(3):
                    p[d, t, h, rows, :] = new[d]
                if total is None or t == 0:
                    continue
                if k == 0:
                    for d in range(3):
                        gu[d, t - 1, h, pl.ds(rows.start - 8, 8), :] = g[d]
                    total = total + length
                else:
                    own = pl.ds(rows.start - 8, 8)
                    if k == 1:
                        s = [g[d] + gu[d, t - 1, h, own, :] for d in range(3)]
                        for d in range(3):
                            gu[d, t - 1, h, own, :] = s[d]
                    else:
                        s = [g[d] + 0.5 * gu[d, t - 1, h, own, :] for d in range(3)]
                    square = s[0] * s[0] + s[1] * s[1] + s[2] * s[2]
                    total = total + square * lax.rsqrt(jnp.maximum(square, TINY))
        return total

    def dual_range(k, b, g0, g1, total):
        def body(g, total):
            rows = rows_of(g)
            nexts, frame_nexts = cn[k, b], tcn[k, b]

            def ghost_of(t):
                if t == 0:
                    return pltpu.roll(frame_nexts, 127 - packed_at(4, g), 1)
                return pltpu.roll(nexts, 127 - packed_at(t, g), 1)

            return dual_group(k, rows, pl.ds(rows.start + 1, 8), range(5), ghost_of, total)

        return grouped(g0, g1, body, total, UNROLL)

    def dual_above(k):
        @pl.when(jnp.logical_not(first_row))
        def _():
            nexts = rcn[k]
            dual_group(
                k, pl.ds(0, 8), pl.ds(1, 8), range(1, 5),
                lambda t: pltpu.roll(nexts, 127 - packed_at(t, 15), 1), None,
            )

    def dual_left(k, b, last):
        here, later_left = cp[k, b], tcp[k, b]
        later = jnp.where(lane >= 48, pltpu.roll(later_left, 48, 1), pltpu.roll(here, 112, 1))
        later = jnp.where(jnp.logical_and(lane >= 48, last_tm), here, later)
        last_group = jnp.bitwise_and(lane, 15) == 15
        follow = pltpu.roll(here, 127, 1)
        if last:
            follow = jnp.where(last_group, pltpu.roll(rcp[k], 15, 1), follow)
        below = jnp.where(sublane == 7, pltpu.roll(follow, 7, 0), pltpu.roll(here, 7, 0))
        bottom = jnp.logical_and(jnp.logical_and(sublane == 7, last_group), last_row)
        below = jnp.where(bottom, here, below)
        g = [later - here, below - here, c0[k, b] - here]
        m = None if k == 0 else [pc[k, d] + SIGMA * g[d] for d in range(3)]
        new, _ = project(k, m, g)
        for d in range(3):
            pc[k + 1, d] = new[d]
        pc[k + 1, 3] = jnp.where(first_col, 0.0, new[2])

    def primal_range(k, g0, g1, total):
        def body(g, total):
            rows = rows_of(g)
            own = pl.ds(rows.start - 8, 8)
            before_rows = pl.ds(rows.start - 1, 8)
            left = pc[k + 1, 3]
            for t in range(1, 5):
                q = [p[2, t, h, rows, :] for h in range(2)]
                rolled = [pltpu.roll(q[h], 1, 1) for h in range(2)]
                ghost = pltpu.roll(left, 128 - packed_at(t, g), 1)
                before = [jnp.where(first_lane, ghost, rolled[0]), jnp.where(first_lane, rolled[0], rolled[1])]
                for h in range(2):
                    e = (
                        (p[0, t, h, rows, :] - p[0, t - 1, h, rows, :])
                        + (p[1, t, h, rows, :] - p[1, t, h, before_rows, :])
                        + (q[h] - before[h])
                    )
                    f = ub[0, t, h, rows, :]
                    scale = damp[t - 1, h, own, :]
                    total = total + (e * e * inv_fid[t - 1, h, own, :] + f * e)
                    if k == 0:
                        new = scale * (TAU * e)
                        bar = f + 2.0 * new
                    else:
                        old = res[t - 1, h, own, :]
                        total = total + old * old * fid[t - 1, h, own, :]
                        new = scale * (old + TAU * e)
                        bar = f + (2.0 * new - old)
                    if k < ITERS - 1:
                        res[t - 1, h, own, :] = new
                        ub[k + 1, t, h, rows, :] = bar
                    else:
                        out_v[t - 1, h, own, :] = f + new
            return total

        return grouped(g0, g1, body, total, UNROLL)

    def weights():
        for load in fid_loads:
            load.wait()

        @pl.loop(0, GROUPS)
        def _(g):
            own = pl.ds(pl.multiple_of(8 * g, 8), 8)
            for t in range(4):
                for h in range(2):
                    lam = fid[t, h, own, :]
                    damp[t, h, own, :] = 1.0 / (1.0 + TAU * lam)
                    inv_fid[t, h, own, :] = 0.5 / lam
                    fid[t, h, own, :] = 0.5 * lam

    for t in (0, 3):
        for h in range(2):
            frame_loads[t, h].wait()
    pl.semaphore_wait(barrier, arrivals)
    for c in range(STEPS):
        start(frame_copies(0, c))
    tell(0)
    for t in (1, 2):
        for h in range(2):
            frame_loads[t, h].wait()
    c0[0, STEPS - 1], c255[0, STEPS - 1] = pack(0, 0, GROUPS, (zero, zero))
    start(low_copies(0) + high_copies(0) + col_copies(0, STEPS - 1))
    weights()
    hear(0)
    tell(1)

    sums = []
    for k in range(ITERS):
        length, total, held = zero, zero, (zero, zero)
        for c in range(STEPS):
            final = c == STEPS - 1
            b = c if k else STEPS - 1
            wait_received(frame_copies(k, c))
            if k or c == 0:
                wait_received(col_copies(k, b))
            if c == ABOVE_STEP[k]:
                wait_received(high_copies(k))
                dual_above(k)
            if final:
                wait_received(low_copies(k))
                hear(k + 1)
                tell(k + 2)

                @pl.when(last_row)
                def _():
                    for t in range(5):
                        for h in range(2):
                            ub[k, t, h, 136:137, :] = ub[k, t, h, 135:136, :]

            dual_left(k, b, final)
            for span in DUAL_STEPS[k][c]:
                length = dual_range(k, b, *span, length)
            for span in PRIMAL_STEPS[k][c]:
                total = primal_range(k, *span, total)
            if k == ITERS - 1:
                continue
            for span in CHUNKS[k + 1][c]:
                held = pack(k + 1, *span, held)
            c0[k + 1, c], c255[k + 1, c] = held
            start(frame_copies(k + 1, c) + col_copies(k + 1, c))
            if c == LOW_CHUNK[k + 1]:
                start(low_copies(k + 1))
            if final:
                start(high_copies(k + 1))
        sums.append(total + (1.0 if k == 0 else 0.5) * length)

    row = jnp.zeros((1, 128), F32)
    row_lane = lax.broadcasted_iota(jnp.int32, (1, 128), 1)
    for k in range(ITERS):
        row = jnp.where(row_lane == k, jnp.sum(sums[k]), row)

    def exchange(mine, slots, me, count, name, i, row):
        mine[...] = row
        slots[me] = row

        @pl.loop(1, count)
        def _(j):
            pltpu.make_async_remote_copy(
                src_ref=mine, dst_ref=slots.at[me], send_sem=ar_send.at[i], recv_sem=ar_recv.at[i],
                device_id=ring(**{name: j}), device_id_type=MESH,
            ).start()

        if i == 0:
            for k in range(ITERS):
                wait_sent(all_copies(k))
        landed = slots.at[pl.ds(0, count - 1)]
        pltpu.make_async_copy(landed, landed, ar_recv.at[i]).wait()
        got = slots[0]
        for j in range(1, count):
            got = got + slots[j]
        return got

    def drain(slots, count, i):
        landed = slots.at[pl.ds(0, count - 1)]
        pltpu.make_async_copy(landed, landed, ar_send.at[i]).wait()

    row = exchange(part.at[0], by_col, at[2], n_col, "col", 0, row)
    row = exchange(part.at[1], by_tm, at[0], n_tm, "tm", 1, row)
    row = exchange(part.at[2], by_row, at[1], n_row, "row", 2, row)
    cells = float(4 * 128 * 256) * float(n_tm * n_row * n_col)
    gaps_ref[...] = row * (1.0 / cells)

    drain(by_col, n_col, 0)
    drain(by_tm, n_tm, 1)
    drain(by_row, n_row, 2)


def put_out(out_v, gaps_ref, out_hbm, gaps_out, sem):
    puts = [pltpu.make_async_copy(out_v.at[:, h], out_hbm.at[:, :, pl.ds(128 * h, 128)], sem.at[h]) for h in range(2)]
    for put in puts:
        put.start()
    for k in range(ITERS):
        gaps_out[k] = gaps_ref[0, k]
    for put in puts:
        put.wait()


def on_device(sizes, noisy_video, fidelity):
    n_chunks = STEPS
    dma = pltpu.SemaphoreType.DMA
    vmem = lambda *shape: pltpu.VMEM(shape, F32)
    out, gaps = pl.pallas_call(
        functools.partial(kernel, sizes),
        out_shape=(vmem(4, 2, 128, 128), vmem(1, 128)),
        in_specs=[pl.BlockSpec(memory_space=pl.ANY)] * 2,
        out_specs=(pl.BlockSpec(memory_space=pltpu.VMEM), pl.BlockSpec(memory_space=pltpu.VMEM)),
        scratch_shapes=[
            vmem(3, 6, 2, 144, 128),
            vmem(3, 5, 2, 136, 128),
            vmem(3, 4, 2, 128, 128),
            vmem(4, 2, 128, 128),
            vmem(4, 2, 128, 128),
            vmem(4, 2, 128, 128),
            vmem(4, 2, 128, 128),
            vmem(3, n_chunks, 8, 128),
            vmem(3, n_chunks, 8, 128),
            vmem(3, n_chunks, 8, 128),
            vmem(3, n_chunks, 8, 128),
            vmem(3, n_chunks, 8, 128),
            vmem(3, n_chunks, 8, 128),
            vmem(3, 8, 128),
            vmem(3, 8, 128),
            vmem(4, 4, 8, 128),
            vmem(3, 1, 128),
            vmem(sizes[2], 1, 128),
            vmem(sizes[0], 1, 128),
            vmem(sizes[1], 1, 128),
            dma((5, 2)),
            dma((3, n_chunks, 2, 2)), dma((3, n_chunks, 2, 2)),
            dma((3, 2)), dma((3, 2)),
            dma((3, n_chunks, 2)), dma((3, n_chunks, 2)),
            dma((3, 2)), dma((3, 2)),
            dma((3, n_chunks, 2)), dma((3, n_chunks, 2)),
            dma((3, 2)), dma((3, 2)),
            dma((3,)), dma((3,)),
            pltpu.SemaphoreType.REGULAR((4, 3)),
        ],
        compiler_params=pltpu.CompilerParams(collective_id=0, has_side_effects=True),
    )(noisy_video, fidelity)
    return pl.pallas_call(
        put_out,
        out_shape=(jax.ShapeDtypeStruct(noisy_video.shape, F32), jax.ShapeDtypeStruct((ITERS,), F32)),
        in_specs=[pl.BlockSpec(memory_space=pltpu.VMEM)] * 2,
        out_specs=(pl.BlockSpec(memory_space=pl.ANY), pl.BlockSpec(memory_space=pltpu.SMEM)),
        scratch_shapes=[dma((2,))],
    )(*(pltpu.with_memory_space_constraint(x, pltpu.VMEM) for x in (out, gaps)))


def solution(mesh):
    sizes = (mesh.shape["tm"], mesh.shape["row"], mesh.shape["col"])
    placed = P("tm", "row", "col")
    return jax.shard_map(
        functools.partial(on_device, sizes),
        mesh=mesh,
        in_specs=(placed, placed),
        out_specs=(placed, P()),
        check_vma=False,
    )
```

```python
import functools
from itertools import zip_longest

import jax
import jax.numpy as jnp
from jax import lax
from jax.experimental import pallas as pl
from jax.experimental.pallas import tpu as pltpu
from jax.sharding import PartitionSpec as P

ITERS = 3
SIGMA = 0.28
TAU = 0.28
TINY = 1.1754943508222875e-38
MESH = pl.DeviceIdType.MESH
F32 = jnp.float32

GROUPS = 16

FRAME_UP, FRAME_DOWN = (1, 0, 0), (-1, 0, 0)
ROW_UP, ROW_DOWN = (0, 1, 0), (0, -1, 0)
COL_UP, COL_DOWN = (0, 0, 1), (0, 0, -1)
NEIGHBOURS = (
    FRAME_UP, FRAME_DOWN, ROW_UP, ROW_DOWN, COL_UP, COL_DOWN,
    (1, -1, 0), (-1, 1, 0), (1, 0, -1), (-1, 0, 1), (0, 1, -1), (0, -1, 1),
)

CUTS = (6, 11)
STEPS = len(CUTS) + 1


def spans(first, back, *more):
    edges = [first] + [cut - back for cut in CUTS] + [16]
    out = [[(a, b)] if b > a else [] for a, b in zip(edges, edges[1:])]
    out[-1] += more
    return out


CHUNKS = (spans(0, -1), spans(0, 0), spans(1, 1, (0, 1)))
DUAL_STEPS = (spans(0, 0), spans(0, 1), spans(1, 2, (0, 1)))
PRIMAL_STEPS = (spans(0, 0), spans(1, 1, (0, 1)), spans(2, 2, (0, 2)))
PHASES = (("x", "tm", "core"), ("row",))
ABOVE_STEP = (0, STEPS - 1, STEPS - 1)
LOW_CHUNK = (STEPS - 1, 0, STEPS - 1)

UNROLL = 4
PACK_UNROLL = 16


def grouped(g0, g1, body, carry, unroll):
    steps = (g1 - g0) // unroll

    def step(i, carry):
        for u in range(unroll):
            carry = body(g0 + i * unroll + u, carry)
        return carry

    if steps > 1:
        carry = lax.fori_loop(0, steps, step, carry)
    elif steps == 1:
        carry = step(0, carry)
    for g in range(g0 + steps * unroll, g1):
        carry = body(g, carry)
    return carry


def rows_of(group):
    start = 8 + 8 * group
    return pl.ds(start if isinstance(start, int) else pl.multiple_of(start, 8), 8)


def kernel(
    sizes, f_hbm, fid_hbm, out_v, gaps_ref,
    ub, p, gu, res, damp, inv_fid, fid, c0, c255, cn, cp, tcn, tcp, rcn, rcp, pc, part, by_phase0, by_phase1, by_phase2,
    load_sem,
    fr_send, fr_recv, row_send, row_recv, col_send, col_recv, tr_send, tr_recv, tc_send, tc_recv, rc_send, rc_recv,
    ar_send, ar_recv, token_sem,
):
    n_tm, n_row, n_col = sizes
    by_phase = (by_phase0, by_phase1, by_phase2)
    at = (lax.axis_index("tm"), lax.axis_index("row"), lax.axis_index("col"))

    def there(step):
        return dict(tm=at[0] + step[0], row=at[1] + step[1], col=at[2] + step[2])

    def exists(step):
        found = None
        for pos, size, move in zip(at, sizes, step):
            if move:
                ok = pos < size - 1 if move > 0 else pos > 0
                found = ok if found is None else jnp.logical_and(found, ok)
        return found

    lane = lax.broadcasted_iota(jnp.int32, (8, 128), 1)
    sublane = lax.broadcasted_iota(jnp.int32, (8, 128), 0)
    first_lane, last_lane = lane == 0, lane == 127
    first_row, first_col, first_tm = at[1] == 0, at[2] == 0, at[0] == 0
    last_row, last_col, last_tm = at[1] == n_row - 1, at[2] == n_col - 1, at[0] == n_tm - 1
    edge_lane = jnp.logical_and(last_lane, last_col)

    frame_loads, fid_loads = {}, []
    for h in range(2):
        cols = pl.ds(128 * h, 128)
        for t in range(4):
            frame_loads[t, h] = pltpu.make_async_copy(
                f_hbm.at[t, :, cols], ub.at[0, t + 1, h, 8:136, :], load_sem.at[t, h])
        fid_loads.append(pltpu.make_async_copy(fid_hbm.at[:, :, cols], fid.at[:, h], load_sem.at[4, h]))
    for t in (0, 3, 1, 2):
        for h in range(2):
            frame_loads[t, h].start()
    for load in fid_loads:
        load.start()

    def ring(**moves):
        out = {}
        for name, pos, size in zip(("tm", "row", "col"), at, sizes):
            out[name] = lax.rem(pos + (moves.get(name, 0) + size), size)
        return out

    barrier = pltpu.get_barrier_semaphore()
    arrivals = 0
    for move in NEIGHBOURS:
        if sum(map(abs, move)) == 1:
            pl.semaphore_signal(
                barrier, inc=1, device_id=ring(tm=move[0], row=move[1], col=move[2]), device_id_type=MESH)
            arrivals = arrivals + 1
            continue
        ok = exists(move)

        @pl.when(ok)
        def _():
            pl.semaphore_signal(barrier, inc=1, device_id=there(move), device_id_type=MESH)

        arrivals = arrivals + ok.astype(jnp.int32)

    def tokens(name, count):
        reach, out = 1, []
        while 2 * reach < count:
            out.append((name, reach))
            reach *= 2
        return out

    of_rows, of_cols = tokens("row", n_row), tokens("col", n_col)
    rounds = list(zip_longest(of_rows, of_cols + [("tm", 1)] * (n_tm // 2)))

    def tell(i):
        for j, token in enumerate(rounds[i] if i < len(rounds) else ()):
            if token:
                name, reach = token
                for d in (reach, -reach):
                    pl.semaphore_signal(
                        token_sem.at[i, j], inc=1, device_id=ring(**{name: d}), device_id_type=MESH)

    def hear(i):
        for j, token in enumerate(rounds[i] if i < len(rounds) else ()):
            if token:
                pl.semaphore_wait(token_sem.at[i, j], 2)

    zero = jnp.zeros((8, 128), F32)

    @pl.when(first_row)
    def _():
        for t in range(1, 5):
            for h in range(2):
                p[1, t, h, 0:8, :] = zero

    def remote(src, dst, send, recv, step):
        return pltpu.make_async_remote_copy(
            src_ref=src, dst_ref=dst, send_sem=send, recv_sem=recv, device_id=there(step), device_id_type=MESH
        )

    def frame_copies(k, c):
        out = []
        for i, (move, src, dst) in enumerate(((FRAME_DOWN, 1, 5), (FRAME_UP, 4, 0))):
            for j, (g0, g1) in enumerate(CHUNKS[k][c]):
                rows = pl.ds(8 + 8 * g0, 8 * (g1 - g0))
                out.append((move, remote(
                    ub.at[k, src, :, rows, :], ub.at[k, dst, :, rows, :],
                    fr_send.at[k, c, i, j], fr_recv.at[k, c, i, j], move)))
        return out

    low, high, ghost_low, ghost_high = pl.ds(8, 1), pl.ds(135, 1), pl.ds(7, 1), pl.ds(136, 1)

    def low_copies(k):
        c = LOW_CHUNK[k]
        return [
            (ROW_DOWN, remote(
                ub.at[k, 1:5, :, low, :], ub.at[k, 1:5, :, ghost_high, :], row_send.at[k, 0], row_recv.at[k, 0], ROW_DOWN)),
            ((1, -1, 0), remote(
                ub.at[k, 4, :, low, :], ub.at[k, 0, :, ghost_high, :], tr_send.at[k, 0], tr_recv.at[k, 0], (1, -1, 0))),
            ((0, -1, 1), remote(c255.at[k, c], rcp.at[k], rc_send.at[k, 1], rc_recv.at[k, 1], (0, -1, 1))),
        ]

    def high_copies(k):
        c = STEPS - 1
        return [
            (ROW_UP, remote(
                ub.at[k, 1:5, :, high, :], ub.at[k, 1:5, :, ghost_low, :], row_send.at[k, 1], row_recv.at[k, 1], ROW_UP)),
            ((-1, 1, 0), remote(
                ub.at[k, 1, :, high, :], ub.at[k, 5, :, ghost_low, :], tr_send.at[k, 1], tr_recv.at[k, 1], (-1, 1, 0))),
            ((0, 1, -1), remote(c0.at[k, c], rcn.at[k], rc_send.at[k, 0], rc_recv.at[k, 0], (0, 1, -1))),
        ]

    def col_copies(k, c):
        return [
            (COL_DOWN, remote(c0.at[k, c], cn.at[k, c], col_send.at[k, c, 0], col_recv.at[k, c, 0], COL_DOWN)),
            (COL_UP, remote(c255.at[k, c], cp.at[k, c], col_send.at[k, c, 1], col_recv.at[k, c, 1], COL_UP)),
            ((1, 0, -1), remote(c0.at[k, c], tcn.at[k, c], tc_send.at[k, c, 0], tc_recv.at[k, c, 0], (1, 0, -1))),
            ((-1, 0, 1), remote(c255.at[k, c], tcp.at[k, c], tc_send.at[k, c, 1], tc_recv.at[k, c, 1], (-1, 0, 1))),
        ]

    def start(copies):
        for step, copy in copies:
            @pl.when(exists(step))
            def _():
                copy.start()

    def wait_sent(copies):
        for step, copy in copies:
            @pl.when(exists(step))
            def _():
                copy.wait_send()

    def wait_received(copies):
        for step, copy in copies:
            @pl.when(exists(tuple(-s for s in step)))
            def _():
                copy.wait_recv()

    def col_chunks(k):
        return range(STEPS) if k else range(STEPS - 1, STEPS)

    def all_copies(k):
        out = low_copies(k) + high_copies(k)
        for c in range(STEPS):
            out += frame_copies(k, c)
        for c in col_chunks(k):
            out += col_copies(k, c)
        return out

    def packed_at(t, g):
        return (t - 1) * 16 + g

    def packed(x0, x1, t, g, held):
        i = packed_at(t, g)
        here = lane == i
        return (
            jnp.where(here, pltpu.roll(x0, i, 1), held[0]),
            jnp.where(here, pltpu.roll(x1, i + 1, 1), held[1]),
        )

    def pack(k, g0, g1, held):
        def body(g, held):
            for t in range(1, 5):
                held = packed(ub[k, t, 0, rows_of(g), :], ub[k, t, 1, rows_of(g), :], t, g, held)
            return held

        return grouped(g0, g1, body, held, PACK_UNROLL)

    def project(k, m, g):
        if k == 0:
            square = g[0] * g[0] + g[1] * g[1] + g[2] * g[2]
            root = lax.rsqrt(jnp.maximum(square, TINY))
            scale = jnp.minimum(SIGMA, root)
            return [g[d] * scale for d in range(3)], square * root
        square = m[0] * m[0] + m[1] * m[1] + m[2] * m[2]
        scale = lax.rsqrt(jnp.maximum(square, 1.0))
        return [m[d] * scale for d in range(3)], None

    def dual_group(k, rows, below, frames, ghost_of, total):
        x = [[ub[k, t, h, rows, :] for h in range(2)] for t in range(frames[0], 6)]
        for t in frames:
            here, later = x[t - frames[0]], x[t - frames[0] + 1]
            if t == 4:
                later = [jnp.where(last_tm, here[h], later[h]) for h in range(2)]
            rolled = [pltpu.roll(here[h], 127, 1) for h in range(2)]
            after = [
                jnp.where(last_lane, rolled[1], rolled[0]),
                jnp.where(edge_lane, here[1], jnp.where(last_lane, ghost_of(t), rolled[1])),
            ]
            for h in range(2):
                g = [later[h] - here[h], ub[k, t, h, below, :] - here[h], after[h] - here[h]]
                m = None if k == 0 else [p[d, t, h, rows, :] + SIGMA * g[d] for d in range(3)]
                new, length = project(k, m, g)
                if t == 0:
                    new[0] = jnp.where(first_tm, 0.0, new[0])
                for d in range(3):
                    p[d, t, h, rows, :] = new[d]
                if total is None or t == 0:
                    continue
                if k == 0:
                    for d in range(3):
                        gu[d, t - 1, h, pl.ds(rows.start - 8, 8), :] = g[d]
                    total = total + length
                else:
                    own = pl.ds(rows.start - 8, 8)
                    if k == 1:
                        s = [g[d] + gu[d, t - 1, h, own, :] for d in range(3)]
                        for d in range(3):
                            gu[d, t - 1, h, own, :] = s[d]
                    else:
                        s = [g[d] + 0.5 * gu[d, t - 1, h, own, :] for d in range(3)]
                    square = s[0] * s[0] + s[1] * s[1] + s[2] * s[2]
                    total = total + square * lax.rsqrt(jnp.maximum(square, TINY))
        return total

    def dual_range(k, b, g0, g1, total):
        def body(g, total):
            rows = rows_of(g)
            nexts, frame_nexts = cn[k, b], tcn[k, b]

            def ghost_of(t):
                if t == 0:
                    return pltpu.roll(frame_nexts, 127 - packed_at(4, g), 1)
                return pltpu.roll(nexts, 127 - packed_at(t, g), 1)

            return dual_group(k, rows, pl.ds(rows.start + 1, 8), range(5), ghost_of, total)

        return grouped(g0, g1, body, total, UNROLL)

    def dual_above(k):
        @pl.when(jnp.logical_not(first_row))
        def _():
            nexts = rcn[k]
            dual_group(
                k, pl.ds(0, 8), pl.ds(1, 8), range(1, 5),
                lambda t: pltpu.roll(nexts, 127 - packed_at(t, 15), 1), None,
            )

    def dual_left(k, b, last):
        here, later_left = cp[k, b], tcp[k, b]
        later = jnp.where(lane >= 48, pltpu.roll(later_left, 48, 1), pltpu.roll(here, 112, 1))
        later = jnp.where(jnp.logical_and(lane >= 48, last_tm), here, later)
        last_group = jnp.bitwise_and(lane, 15) == 15
        follow = pltpu.roll(here, 127, 1)
        if last:
            follow = jnp.where(last_group, pltpu.roll(rcp[k], 15, 1), follow)
        below = jnp.where(sublane == 7, pltpu.roll(follow, 7, 0), pltpu.roll(here, 7, 0))
        bottom = jnp.logical_and(jnp.logical_and(sublane == 7, last_group), last_row)
        below = jnp.where(bottom, here, below)
        g = [later - here, below - here, c0[k, b] - here]
        m = None if k == 0 else [pc[k, d] + SIGMA * g[d] for d in range(3)]
        new, _ = project(k, m, g)
        for d in range(3):
            pc[k + 1, d] = new[d]
        pc[k + 1, 3] = jnp.where(first_col, 0.0, new[2])

    def primal_range(k, g0, g1, total):
        def body(g, total):
            rows = rows_of(g)
            own = pl.ds(rows.start - 8, 8)
            before_rows = pl.ds(rows.start - 1, 8)
            left = pc[k + 1, 3]
            for t in range(1, 5):
                q = [p[2, t, h, rows, :] for h in range(2)]
                rolled = [pltpu.roll(q[h], 1, 1) for h in range(2)]
                ghost = pltpu.roll(left, 128 - packed_at(t, g), 1)
                before = [jnp.where(first_lane, ghost, rolled[0]), jnp.where(first_lane, rolled[0], rolled[1])]
                for h in range(2):
                    e = (
                        (p[0, t, h, rows, :] - p[0, t - 1, h, rows, :])
                        + (p[1, t, h, rows, :] - p[1, t, h, before_rows, :])
                        + (q[h] - before[h])
                    )
                    f = ub[0, t, h, rows, :]
                    scale = damp[t - 1, h, own, :]
                    total = total + (e * e * inv_fid[t - 1, h, own, :] + f * e)
                    if k == 0:
                        new = scale * (TAU * e)
                        bar = f + 2.0 * new
                    else:
                        old = res[t - 1, h, own, :]
                        total = total + old * old * fid[t - 1, h, own, :]
                        new = scale * (old + TAU * e)
                        bar = f + (2.0 * new - old)
                    if k < ITERS - 1:
                        res[t - 1, h, own, :] = new
                        ub[k + 1, t, h, rows, :] = bar
                    else:
                        out_v[t - 1, h, own, :] = f + new
            return total

        return grouped(g0, g1, body, total, UNROLL)

    def weights():
        for load in fid_loads:
            load.wait()

        @pl.loop(0, GROUPS)
        def _(g):
            own = pl.ds(pl.multiple_of(8 * g, 8), 8)
            for t in range(4):
                for h in range(2):
                    lam = fid[t, h, own, :]
                    damp[t, h, own, :] = 1.0 / (1.0 + TAU * lam)
                    inv_fid[t, h, own, :] = 0.5 / lam
                    fid[t, h, own, :] = 0.5 * lam

    for load in frame_loads.values():
        load.wait()
    c0[0, STEPS - 1], c255[0, STEPS - 1] = pack(0, 0, GROUPS, (zero, zero))
    pl.semaphore_wait(barrier, arrivals)
    start(col_copies(0, STEPS - 1))
    start(frame_copies(0, 0))
    start(low_copies(0) + high_copies(0))
    tell(0)
    for c in range(1, STEPS):
        start(frame_copies(0, c))
    weights()
    hear(0)
    tell(1)

    row = jnp.zeros((1, 128), F32)
    row_lane = lax.broadcasted_iota(jnp.int32, (1, 128), 1)
    for k in range(ITERS):
        length, total, held = zero, zero, (zero, zero)
        for c in range(STEPS):
            final = c == STEPS - 1
            b = c if k else STEPS - 1
            wait_received(frame_copies(k, c))
            if k or c == 0:
                wait_received(col_copies(k, b))
            if c == ABOVE_STEP[k]:
                wait_received(high_copies(k))
                dual_above(k)
            if final:
                wait_received(low_copies(k))
                hear(k + 1)
                tell(k + 2)

                @pl.when(last_row)
                def _():
                    for t in range(5):
                        for h in range(2):
                            ub[k, t, h, 136:137, :] = ub[k, t, h, 135:136, :]

            dual_left(k, b, final)
            for span in DUAL_STEPS[k][c]:
                length = dual_range(k, b, *span, length)
            for span in PRIMAL_STEPS[k][c]:
                total = primal_range(k, *span, total)
            if k == ITERS - 1:
                continue
            for span in CHUNKS[k + 1][c]:
                held = pack(k + 1, *span, held)
            c0[k + 1, c], c255[k + 1, c] = held
            start(col_copies(k + 1, c))
            if c == LOW_CHUNK[k + 1]:
                start(low_copies(k + 1))
            if final:
                start(high_copies(k + 1))
            start(frame_copies(k + 1, c))
        row = jnp.where(row_lane == k, jnp.sum(total + (1.0 if k == 0 else 0.5) * length), row)

    places = {"tm": (at[0], n_tm), "row": (at[1], n_row), "x": (at[2] // 2, n_col // 2), "core": (at[2] % 2, 2)}

    def exchange(i, axes, row):
        slots, count, me = by_phase[i], 1, 0
        for name in axes:
            pos, size = places[name]
            count, me = count * size, me * size + pos
        part[i] = row
        slots[me] = row

        def tell_one(j):
            there, left = {name: places[name][0] for name in places}, j
            for name in reversed(axes):
                size = places[name][1]
                there[name] = jnp.bitwise_xor(there[name], jnp.bitwise_and(left, size - 1))
                left = jnp.right_shift(left, size.bit_length() - 1)
            pltpu.make_async_remote_copy(
                src_ref=part.at[i], dst_ref=slots.at[me], send_sem=ar_send.at[i], recv_sem=ar_recv.at[i],
                device_id=dict(tm=there["tm"], row=there["row"], col=there["x"] * 2 + there["core"]),
                device_id_type=MESH,
            ).start()

        if count <= 16:
            for j in range(1, count):
                tell_one(j)
        else:
            pl.loop(1, count)(tell_one)

        if i == 0:
            for k in range(ITERS):
                wait_sent(all_copies(k))
        landed = slots.at[pl.ds(0, count - 1)]
        pltpu.make_async_copy(landed, landed, ar_recv.at[i]).wait()
        got = [slots[j] for j in range(count)]
        while len(got) > 1:
            got = [got[j] + got[j + 1] for j in range(0, len(got), 2)]
        return got[0]

    def drain(i, axes):
        count = 1
        for name in axes:
            count *= places[name][1]
        landed = by_phase[i].at[pl.ds(0, count - 1)]
        pltpu.make_async_copy(landed, landed, ar_send.at[i]).wait()

    for i, axes in enumerate(PHASES):
        row = exchange(i, axes, row)
    cells = float(4 * 128 * 256) * float(n_tm * n_row * n_col)
    gaps_ref[...] = row * (1.0 / cells)

    for i, axes in enumerate(PHASES):
        drain(i, axes)


def put_out(out_v, gaps_ref, out_hbm, gaps_out, sem):
    puts = [pltpu.make_async_copy(out_v.at[:, h], out_hbm.at[:, :, pl.ds(128 * h, 128)], sem.at[h]) for h in range(2)]
    for put in puts:
        put.start()
    for k in range(ITERS):
        gaps_out[k] = gaps_ref[0, k]
    for put in puts:
        put.wait()


def on_device(sizes, noisy_video, fidelity):
    n_chunks = STEPS
    dma = pltpu.SemaphoreType.DMA
    vmem = lambda *shape: pltpu.VMEM(shape, F32)
    out, gaps = pl.pallas_call(
        functools.partial(kernel, sizes),
        out_shape=(vmem(4, 2, 128, 128), vmem(1, 128)),
        in_specs=[pl.BlockSpec(memory_space=pl.ANY)] * 2,
        out_specs=(pl.BlockSpec(memory_space=pltpu.VMEM), pl.BlockSpec(memory_space=pltpu.VMEM)),
        scratch_shapes=[
            vmem(3, 6, 2, 144, 128),
            vmem(3, 5, 2, 136, 128),
            vmem(3, 4, 2, 128, 128),
            vmem(4, 2, 128, 128),
            vmem(4, 2, 128, 128),
            vmem(4, 2, 128, 128),
            vmem(4, 2, 128, 128),
            vmem(3, n_chunks, 8, 128),
            vmem(3, n_chunks, 8, 128),
            vmem(3, n_chunks, 8, 128),
            vmem(3, n_chunks, 8, 128),
            vmem(3, n_chunks, 8, 128),
            vmem(3, n_chunks, 8, 128),
            vmem(3, 8, 128),
            vmem(3, 8, 128),
            vmem(4, 4, 8, 128),
            vmem(3, 1, 128),
            vmem(64, 1, 128),
            vmem(64, 1, 128),
            vmem(64, 1, 128),
            dma((5, 2)),
            dma((3, n_chunks, 2, 2)), dma((3, n_chunks, 2, 2)),
            dma((3, 2)), dma((3, 2)),
            dma((3, n_chunks, 2)), dma((3, n_chunks, 2)),
            dma((3, 2)), dma((3, 2)),
            dma((3, n_chunks, 2)), dma((3, n_chunks, 2)),
            dma((3, 2)), dma((3, 2)),
            dma((3,)), dma((3,)),
            pltpu.SemaphoreType.REGULAR((4, 3)),
        ],
        compiler_params=pltpu.CompilerParams(collective_id=0, has_side_effects=True),
    )(noisy_video, fidelity)
    return pl.pallas_call(
        put_out,
        out_shape=(jax.ShapeDtypeStruct(noisy_video.shape, F32), jax.ShapeDtypeStruct((ITERS,), F32)),
        in_specs=[pl.BlockSpec(memory_space=pltpu.VMEM)] * 2,
        out_specs=(pl.BlockSpec(memory_space=pl.ANY), pl.BlockSpec(memory_space=pltpu.SMEM)),
        scratch_shapes=[dma((2,))],
    )(*(pltpu.with_memory_space_constraint(x, pltpu.VMEM) for x in (out, gaps)))


def solution(mesh):
    sizes = (mesh.shape["tm"], mesh.shape["row"], mesh.shape["col"])
    placed = P("tm", "row", "col")
    return jax.shard_map(
        functools.partial(on_device, sizes),
        mesh=mesh,
        in_specs=(placed, placed),
        out_specs=(placed, P()),
        check_vma=False,
    )
```

```python
import functools
from itertools import zip_longest

import jax
import jax.numpy as jnp
from jax import lax
from jax.experimental import pallas as pl
from jax.experimental.pallas import tpu as pltpu
from jax.sharding import PartitionSpec as P

ITERS = 3
SIGMA = 0.28
TAU = 0.28
TINY = 1.1754943508222875e-38
MESH = pl.DeviceIdType.MESH
F32 = jnp.float32

GROUPS = 16

FRAME_UP, FRAME_DOWN = (1, 0, 0), (-1, 0, 0)
ROW_UP, ROW_DOWN = (0, 1, 0), (0, -1, 0)
COL_UP, COL_DOWN = (0, 0, 1), (0, 0, -1)
NEIGHBOURS = (
    FRAME_UP, FRAME_DOWN, ROW_UP, ROW_DOWN, COL_UP, COL_DOWN,
    (1, -1, 0), (-1, 1, 0), (1, 0, -1), (-1, 0, 1), (0, 1, -1), (0, -1, 1),
)

CUTS = (5, 11)
STEPS = len(CUTS) + 1


def spans(first, back, *more):
    edges = [first] + [cut - back for cut in CUTS] + [16]
    out = [[(a, b)] if b > a else [] for a, b in zip(edges, edges[1:])]
    out[-1] += more
    return out


CHUNKS = (spans(0, -1), spans(0, 0), spans(1, 1, (0, 1)))
DUAL_STEPS = (spans(0, 0), spans(0, 1), spans(1, 2, (0, 1)))
PRIMAL_STEPS = (spans(0, 0), spans(1, 1, (0, 1)), spans(2, 2, (0, 2)))
PHASES = (("x", "tm", "core"), ("row",))
ABOVE_STEP = (0, STEPS - 1, STEPS - 1)
LOW_CHUNK = (STEPS - 1, 0, STEPS - 1)

UNROLL = 4
PACK_UNROLL = 16


def grouped(g0, g1, body, carry, unroll):
    steps = (g1 - g0) // unroll

    def step(i, carry):
        for u in range(unroll):
            carry = body(g0 + i * unroll + u, carry)
        return carry

    if steps > 1:
        carry = lax.fori_loop(0, steps, step, carry)
    elif steps == 1:
        carry = step(0, carry)
    for g in range(g0 + steps * unroll, g1):
        carry = body(g, carry)
    return carry


def rows_of(group):
    start = 8 + 8 * group
    return pl.ds(start if isinstance(start, int) else pl.multiple_of(start, 8), 8)


def kernel(
    sizes, f_hbm, fid_hbm, out_v, gaps_ref,
    ub, p, gu, res, damp, inv_fid, fid, c0, c255, cn, cp, tcn, tcp, rcn, rcp, pc, part, by_phase0, by_phase1, by_phase2,
    load_sem,
    fr_send, fr_recv, row_send, row_recv, col_send, col_recv, tr_send, tr_recv, tc_send, tc_recv, rc_send, rc_recv,
    ar_send, ar_recv, token_sem,
):
    n_tm, n_row, n_col = sizes
    by_phase = (by_phase0, by_phase1, by_phase2)
    at = (lax.axis_index("tm"), lax.axis_index("row"), lax.axis_index("col"))

    def there(step):
        return dict(tm=at[0] + step[0], row=at[1] + step[1], col=at[2] + step[2])

    def exists(step):
        found = None
        for pos, size, move in zip(at, sizes, step):
            if move:
                ok = pos < size - 1 if move > 0 else pos > 0
                found = ok if found is None else jnp.logical_and(found, ok)
        return found

    lane = lax.broadcasted_iota(jnp.int32, (8, 128), 1)
    sublane = lax.broadcasted_iota(jnp.int32, (8, 128), 0)
    first_lane, last_lane = lane == 0, lane == 127
    first_row, first_col, first_tm = at[1] == 0, at[2] == 0, at[0] == 0
    last_row, last_col, last_tm = at[1] == n_row - 1, at[2] == n_col - 1, at[0] == n_tm - 1
    edge_lane = jnp.logical_and(last_lane, last_col)

    frame_loads, fid_loads = {}, []
    for h in range(2):
        cols = pl.ds(128 * h, 128)
        for t in range(4):
            frame_loads[t, h] = pltpu.make_async_copy(
                f_hbm.at[t, :, cols], ub.at[0, t + 1, h, 8:136, :], load_sem.at[t, h])
        fid_loads.append(pltpu.make_async_copy(fid_hbm.at[:, :, cols], fid.at[:, h], load_sem.at[4, h]))
    for t in (0, 3, 1, 2):
        for h in range(2):
            frame_loads[t, h].start()
    for load in fid_loads:
        load.start()

    def ring(**moves):
        out = {}
        for name, pos, size in zip(("tm", "row", "col"), at, sizes):
            out[name] = lax.rem(pos + (moves.get(name, 0) + size), size)
        return out

    barrier = pltpu.get_barrier_semaphore()
    arrivals = 0
    for move in NEIGHBOURS:
        if sum(map(abs, move)) == 1:
            pl.semaphore_signal(
                barrier, inc=1, device_id=ring(tm=move[0], row=move[1], col=move[2]), device_id_type=MESH)
            arrivals = arrivals + 1
            continue
        ok = exists(move)

        @pl.when(ok)
        def _():
            pl.semaphore_signal(barrier, inc=1, device_id=there(move), device_id_type=MESH)

        arrivals = arrivals + ok.astype(jnp.int32)

    def tokens(name, count):
        reach, out = 1, []
        while 2 * reach < count:
            out.append((name, reach))
            reach *= 2
        return out

    of_rows, of_cols = tokens("row", n_row), tokens("col", n_col)
    rounds = list(zip_longest(of_rows, of_cols + [("tm", 1)] * (n_tm // 2)))

    def tell(i):
        for j, token in enumerate(rounds[i] if i < len(rounds) else ()):
            if token:
                name, reach = token
                for d in (reach, -reach):
                    pl.semaphore_signal(
                        token_sem.at[i, j], inc=1, device_id=ring(**{name: d}), device_id_type=MESH)

    def hear(i):
        for j, token in enumerate(rounds[i] if i < len(rounds) else ()):
            if token:
                pl.semaphore_wait(token_sem.at[i, j], 2)

    zero = jnp.zeros((8, 128), F32)

    @pl.when(first_row)
    def _():
        for t in range(1, 5):
            for h in range(2):
                p[1, t, h, 0:8, :] = zero

    def remote(src, dst, send, recv, step):
        return pltpu.make_async_remote_copy(
            src_ref=src, dst_ref=dst, send_sem=send, recv_sem=recv, device_id=there(step), device_id_type=MESH
        )

    def frame_copies(k, c):
        out = []
        for i, (move, src, dst) in enumerate(((FRAME_DOWN, 1, 5), (FRAME_UP, 4, 0))):
            for j, (g0, g1) in enumerate(CHUNKS[k][c]):
                rows = pl.ds(8 + 8 * g0, 8 * (g1 - g0))
                out.append((move, remote(
                    ub.at[k, src, :, rows, :], ub.at[k, dst, :, rows, :],
                    fr_send.at[k, c, i, j], fr_recv.at[k, c, i, j], move)))
        return out

    low, high, ghost_low, ghost_high = pl.ds(8, 1), pl.ds(135, 1), pl.ds(7, 1), pl.ds(136, 1)

    def low_copies(k):
        c = LOW_CHUNK[k]
        return [
            (ROW_DOWN, remote(
                ub.at[k, 1:5, :, low, :], ub.at[k, 1:5, :, ghost_high, :], row_send.at[k, 0], row_recv.at[k, 0], ROW_DOWN)),
            ((1, -1, 0), remote(
                ub.at[k, 4, :, low, :], ub.at[k, 0, :, ghost_high, :], tr_send.at[k, 0], tr_recv.at[k, 0], (1, -1, 0))),
            ((0, -1, 1), remote(c255.at[k, c], rcp.at[k], rc_send.at[k, 1], rc_recv.at[k, 1], (0, -1, 1))),
        ]

    def high_copies(k):
        c = STEPS - 1
        return [
            (ROW_UP, remote(
                ub.at[k, 1:5, :, high, :], ub.at[k, 1:5, :, ghost_low, :], row_send.at[k, 1], row_recv.at[k, 1], ROW_UP)),
            ((-1, 1, 0), remote(
                ub.at[k, 1, :, high, :], ub.at[k, 5, :, ghost_low, :], tr_send.at[k, 1], tr_recv.at[k, 1], (-1, 1, 0))),
            ((0, 1, -1), remote(c0.at[k, c], rcn.at[k], rc_send.at[k, 0], rc_recv.at[k, 0], (0, 1, -1))),
        ]

    def col_copies(k, c):
        return [
            (COL_DOWN, remote(c0.at[k, c], cn.at[k, c], col_send.at[k, c, 0], col_recv.at[k, c, 0], COL_DOWN)),
            (COL_UP, remote(c255.at[k, c], cp.at[k, c], col_send.at[k, c, 1], col_recv.at[k, c, 1], COL_UP)),
            ((1, 0, -1), remote(c0.at[k, c], tcn.at[k, c], tc_send.at[k, c, 0], tc_recv.at[k, c, 0], (1, 0, -1))),
            ((-1, 0, 1), remote(c255.at[k, c], tcp.at[k, c], tc_send.at[k, c, 1], tc_recv.at[k, c, 1], (-1, 0, 1))),
        ]

    def start(copies):
        for step, copy in copies:
            @pl.when(exists(step))
            def _():
                copy.start()

    def wait_sent(copies):
        for step, copy in copies:
            @pl.when(exists(step))
            def _():
                copy.wait_send()

    def wait_received(copies):
        for step, copy in copies:
            @pl.when(exists(tuple(-s for s in step)))
            def _():
                copy.wait_recv()

    def col_chunks(k):
        return range(STEPS) if k else range(STEPS - 1, STEPS)

    def all_copies(k):
        out = low_copies(k) + high_copies(k)
        for c in range(STEPS):
            out += frame_copies(k, c)
        for c in col_chunks(k):
            out += col_copies(k, c)
        return out

    def packed_at(t, g):
        return (t - 1) * 16 + g

    def packed(x0, x1, t, g, held):
        i = packed_at(t, g)
        here = lane == i
        return (
            jnp.where(here, pltpu.roll(x0, i, 1), held[0]),
            jnp.where(here, pltpu.roll(x1, i + 1, 1), held[1]),
        )

    def pack(k, g0, g1, held):
        def body(g, held):
            for t in range(1, 5):
                held = packed(ub[k, t, 0, rows_of(g), :], ub[k, t, 1, rows_of(g), :], t, g, held)
            return held

        return grouped(g0, g1, body, held, PACK_UNROLL)

    def project(k, m, g):
        if k == 0:
            square = g[0] * g[0] + g[1] * g[1] + g[2] * g[2]
            root = lax.rsqrt(jnp.maximum(square, TINY))
            scale = jnp.minimum(SIGMA, root)
            return [g[d] * scale for d in range(3)], square * root
        square = m[0] * m[0] + m[1] * m[1] + m[2] * m[2]
        scale = lax.rsqrt(jnp.maximum(square, 1.0))
        return [m[d] * scale for d in range(3)], None

    def dual_group(k, rows, below, frames, ghost_of, total):
        x = [[ub[k, t, h, rows, :] for h in range(2)] for t in range(frames[0], 6)]
        for t in frames:
            here, later = x[t - frames[0]], x[t - frames[0] + 1]
            if t == 4:
                later = [jnp.where(last_tm, here[h], later[h]) for h in range(2)]
            rolled = [pltpu.roll(here[h], 127, 1) for h in range(2)]
            after = [
                jnp.where(last_lane, rolled[1], rolled[0]),
                jnp.where(edge_lane, here[1], jnp.where(last_lane, ghost_of(t), rolled[1])),
            ]
            for h in range(2):
                g = [later[h] - here[h], ub[k, t, h, below, :] - here[h], after[h] - here[h]]
                m = None if k == 0 else [p[d, t, h, rows, :] + SIGMA * g[d] for d in range(3)]
                new, length = project(k, m, g)
                if t == 0:
                    new[0] = jnp.where(first_tm, 0.0, new[0])
                for d in range(3):
                    p[d, t, h, rows, :] = new[d]
                if total is None or t == 0:
                    continue
                if k == 0:
                    for d in range(3):
                        gu[d, t - 1, h, pl.ds(rows.start - 8, 8), :] = g[d]
                    total = total + length
                else:
                    own = pl.ds(rows.start - 8, 8)
                    if k == 1:
                        s = [g[d] + gu[d, t - 1, h, own, :] for d in range(3)]
                        for d in range(3):
                            gu[d, t - 1, h, own, :] = s[d]
                    else:
                        s = [g[d] + 0.5 * gu[d, t - 1, h, own, :] for d in range(3)]
                    square = s[0] * s[0] + s[1] * s[1] + s[2] * s[2]
                    total = total + square * lax.rsqrt(jnp.maximum(square, TINY))
        return total

    def dual_range(k, b, g0, g1, total):
        def body(g, total):
            rows = rows_of(g)
            nexts, frame_nexts = cn[k, b], tcn[k, b]

            def ghost_of(t):
                if t == 0:
                    return pltpu.roll(frame_nexts, 127 - packed_at(4, g), 1)
                return pltpu.roll(nexts, 127 - packed_at(t, g), 1)

            return dual_group(k, rows, pl.ds(rows.start + 1, 8), range(5), ghost_of, total)

        return grouped(g0, g1, body, total, UNROLL)

    def dual_above(k):
        @pl.when(jnp.logical_not(first_row))
        def _():
            nexts = rcn[k]
            dual_group(
                k, pl.ds(0, 8), pl.ds(1, 8), range(1, 5),
                lambda t: pltpu.roll(nexts, 127 - packed_at(t, 15), 1), None,
            )

    def dual_left(k, b, last):
        here, later_left = cp[k, b], tcp[k, b]
        later = jnp.where(lane >= 48, pltpu.roll(later_left, 48, 1), pltpu.roll(here, 112, 1))
        later = jnp.where(jnp.logical_and(lane >= 48, last_tm), here, later)
        last_group = jnp.bitwise_and(lane, 15) == 15
        follow = pltpu.roll(here, 127, 1)
        if last:
            follow = jnp.where(last_group, pltpu.roll(rcp[k], 15, 1), follow)
        below = jnp.where(sublane == 7, pltpu.roll(follow, 7, 0), pltpu.roll(here, 7, 0))
        bottom = jnp.logical_and(jnp.logical_and(sublane == 7, last_group), last_row)
        below = jnp.where(bottom, here, below)
        g = [later - here, below - here, c0[k, b] - here]
        m = None if k == 0 else [pc[k, d] + SIGMA * g[d] for d in range(3)]
        new, _ = project(k, m, g)
        for d in range(3):
            pc[k + 1, d] = new[d]
        pc[k + 1, 3] = jnp.where(first_col, 0.0, new[2])

    def primal_range(k, g0, g1, total):
        def body(g, total):
            rows = rows_of(g)
            own = pl.ds(rows.start - 8, 8)
            before_rows = pl.ds(rows.start - 1, 8)
            left = pc[k + 1, 3]
            for t in range(1, 5):
                q = [p[2, t, h, rows, :] for h in range(2)]
                rolled = [pltpu.roll(q[h], 1, 1) for h in range(2)]
                ghost = pltpu.roll(left, 128 - packed_at(t, g), 1)
                before = [jnp.where(first_lane, ghost, rolled[0]), jnp.where(first_lane, rolled[0], rolled[1])]
                for h in range(2):
                    e = (
                        (p[0, t, h, rows, :] - p[0, t - 1, h, rows, :])
                        + (p[1, t, h, rows, :] - p[1, t, h, before_rows, :])
                        + (q[h] - before[h])
                    )
                    f = ub[0, t, h, rows, :]
                    scale = damp[t - 1, h, own, :]
                    total = total + (e * e * inv_fid[t - 1, h, own, :] + f * e)
                    if k == 0:
                        new = scale * (TAU * e)
                        bar = f + 2.0 * new
                    else:
                        old = res[t - 1, h, own, :]
                        total = total + old * old * fid[t - 1, h, own, :]
                        new = scale * (old + TAU * e)
                        bar = f + (2.0 * new - old)
                    if k < ITERS - 1:
                        res[t - 1, h, own, :] = new
                        ub[k + 1, t, h, rows, :] = bar
                    else:
                        out_v[t - 1, h, own, :] = f + new
            return total

        return grouped(g0, g1, body, total, UNROLL)

    def weights():
        for load in fid_loads:
            load.wait()

        @pl.loop(0, GROUPS)
        def _(g):
            own = pl.ds(pl.multiple_of(8 * g, 8), 8)
            for t in range(4):
                for h in range(2):
                    lam = fid[t, h, own, :]
                    damp[t, h, own, :] = 1.0 / (1.0 + TAU * lam)
                    inv_fid[t, h, own, :] = 0.5 / lam
                    fid[t, h, own, :] = 0.5 * lam

    for load in frame_loads.values():
        load.wait()
    c0[0, STEPS - 1], c255[0, STEPS - 1] = pack(0, 0, GROUPS, (zero, zero))
    pl.semaphore_wait(barrier, arrivals)
    start(col_copies(0, STEPS - 1))
    start(frame_copies(0, 0))
    start(low_copies(0) + high_copies(0))
    tell(0)
    for c in range(1, STEPS):
        start(frame_copies(0, c))
    weights()
    hear(0)
    tell(1)

    row = jnp.zeros((1, 128), F32)
    row_lane = lax.broadcasted_iota(jnp.int32, (1, 128), 1)
    for k in range(ITERS):
        length, total, held = zero, zero, (zero, zero)
        for c in range(STEPS):
            final = c == STEPS - 1
            b = c if k else STEPS - 1
            wait_received(frame_copies(k, c))
            if k or c == 0:
                wait_received(col_copies(k, b))
            if c == ABOVE_STEP[k]:
                wait_received(high_copies(k))
                dual_above(k)
            if final:
                wait_received(low_copies(k))
                hear(k + 1)
                tell(k + 2)

                @pl.when(last_row)
                def _():
                    for t in range(5):
                        for h in range(2):
                            ub[k, t, h, 136:137, :] = ub[k, t, h, 135:136, :]

            dual_left(k, b, final)
            for span in DUAL_STEPS[k][c]:
                length = dual_range(k, b, *span, length)
            for span in PRIMAL_STEPS[k][c]:
                total = primal_range(k, *span, total)
            if k == ITERS - 1:
                continue
            for span in CHUNKS[k + 1][c]:
                held = pack(k + 1, *span, held)
            c0[k + 1, c], c255[k + 1, c] = held
            start(col_copies(k + 1, c))
            if c == LOW_CHUNK[k + 1]:
                start(low_copies(k + 1))
            if final:
                start(high_copies(k + 1))
            start(frame_copies(k + 1, c))
        row = jnp.where(row_lane == k, jnp.sum(total + (1.0 if k == 0 else 0.5) * length), row)

    places = {"tm": (at[0], n_tm), "row": (at[1], n_row), "x": (at[2] // 2, n_col // 2), "core": (at[2] % 2, 2)}

    def exchange(i, axes, row):
        slots, count, me = by_phase[i], 1, 0
        for name in axes:
            pos, size = places[name]
            count, me = count * size, me * size + pos
        part[i] = row
        slots[me] = row

        def tell_one(j):
            there, left = {name: places[name][0] for name in places}, j
            for name in reversed(axes):
                size = places[name][1]
                there[name] = jnp.bitwise_xor(there[name], jnp.bitwise_and(left, size - 1))
                left = jnp.right_shift(left, size.bit_length() - 1)
            pltpu.make_async_remote_copy(
                src_ref=part.at[i], dst_ref=slots.at[me], send_sem=ar_send.at[i], recv_sem=ar_recv.at[i],
                device_id=dict(tm=there["tm"], row=there["row"], col=there["x"] * 2 + there["core"]),
                device_id_type=MESH,
            ).start()

        if count <= 16:
            for j in range(1, count):
                tell_one(j)
        else:
            pl.loop(1, count)(tell_one)

        if i == 0:
            for k in range(ITERS):
                wait_sent(all_copies(k))
        landed = slots.at[pl.ds(0, count - 1)]
        pltpu.make_async_copy(landed, landed, ar_recv.at[i]).wait()
        got = [slots[j] for j in range(count)]
        while len(got) > 1:
            got = [got[j] + got[j + 1] for j in range(0, len(got), 2)]
        return got[0]

    def drain(i, axes):
        count = 1
        for name in axes:
            count *= places[name][1]
        landed = by_phase[i].at[pl.ds(0, count - 1)]
        pltpu.make_async_copy(landed, landed, ar_send.at[i]).wait()

    for i, axes in enumerate(PHASES):
        row = exchange(i, axes, row)
    cells = float(4 * 128 * 256) * float(n_tm * n_row * n_col)
    gaps_ref[...] = row * (1.0 / cells)

    for i, axes in enumerate(PHASES):
        drain(i, axes)


def put_out(out_v, gaps_ref, out_hbm, gaps_out, sem, gaps_s):
    puts = [pltpu.make_async_copy(out_v.at[:, h], out_hbm.at[:, :, pl.ds(128 * h, 128)], sem.at[h]) for h in range(2)]
    for put in puts:
        put.start()
    for k in range(ITERS):
        gaps_s[k] = gaps_ref[0, k]
    last = pltpu.make_async_copy(gaps_s, gaps_out, sem.at[2])
    last.start()
    puts.append(last)
    for put in puts:
        put.wait()


def on_device(sizes, noisy_video, fidelity):
    n_chunks = STEPS
    dma = pltpu.SemaphoreType.DMA
    vmem = lambda *shape: pltpu.VMEM(shape, F32)
    out, gaps = pl.pallas_call(
        functools.partial(kernel, sizes),
        out_shape=(vmem(4, 2, 128, 128), vmem(1, 128)),
        in_specs=[pl.BlockSpec(memory_space=pl.ANY)] * 2,
        out_specs=(pl.BlockSpec(memory_space=pltpu.VMEM), pl.BlockSpec(memory_space=pltpu.VMEM)),
        scratch_shapes=[
            vmem(3, 6, 2, 144, 128),
            vmem(3, 5, 2, 136, 128),
            vmem(3, 4, 2, 128, 128),
            vmem(4, 2, 128, 128),
            vmem(4, 2, 128, 128),
            vmem(4, 2, 128, 128),
            vmem(4, 2, 128, 128),
            vmem(3, n_chunks, 8, 128),
            vmem(3, n_chunks, 8, 128),
            vmem(3, n_chunks, 8, 128),
            vmem(3, n_chunks, 8, 128),
            vmem(3, n_chunks, 8, 128),
            vmem(3, n_chunks, 8, 128),
            vmem(3, 8, 128),
            vmem(3, 8, 128),
            vmem(4, 4, 8, 128),
            vmem(3, 1, 128),
            vmem(64, 1, 128),
            vmem(64, 1, 128),
            vmem(64, 1, 128),
            dma((5, 2)),
            dma((3, n_chunks, 2, 2)), dma((3, n_chunks, 2, 2)),
            dma((3, 2)), dma((3, 2)),
            dma((3, n_chunks, 2)), dma((3, n_chunks, 2)),
            dma((3, 2)), dma((3, 2)),
            dma((3, n_chunks, 2)), dma((3, n_chunks, 2)),
            dma((3, 2)), dma((3, 2)),
            dma((3,)), dma((3,)),
            pltpu.SemaphoreType.REGULAR((4, 3)),
        ],
        compiler_params=pltpu.CompilerParams(collective_id=0, has_side_effects=True),
    )(noisy_video, fidelity)
    return pl.pallas_call(
        put_out,
        out_shape=(jax.ShapeDtypeStruct(noisy_video.shape, F32), jax.ShapeDtypeStruct((ITERS,), F32)),
        in_specs=[pl.BlockSpec(memory_space=pltpu.VMEM)] * 2,
        out_specs=(pl.BlockSpec(memory_space=pl.ANY), pl.BlockSpec(memory_space=pl.ANY)),
        scratch_shapes=[dma((3,)), pltpu.SMEM((ITERS,), F32)],
    )(*(pltpu.with_memory_space_constraint(x, pltpu.VMEM) for x in (out, gaps)))


def solution(mesh):
    sizes = (mesh.shape["tm"], mesh.shape["row"], mesh.shape["col"])
    placed = P("tm", "row", "col")
    return jax.shard_map(
        functools.partial(on_device, sizes),
        mesh=mesh,
        in_specs=(placed, placed),
        out_specs=(placed, P()),
        check_vma=False,
    )
```

```python
import functools
from itertools import zip_longest

import jax
import jax.numpy as jnp
from jax import lax
from jax.experimental import pallas as pl
from jax.experimental.pallas import tpu as pltpu
from jax.sharding import PartitionSpec as P

ITERS = 3
SIGMA = 0.28
TAU = 0.28
TINY = 1.1754943508222875e-38
MESH = pl.DeviceIdType.MESH
F32 = jnp.float32

GROUPS = 16

FRAME_UP, FRAME_DOWN = (1, 0, 0), (-1, 0, 0)
ROW_UP, ROW_DOWN = (0, 1, 0), (0, -1, 0)
COL_UP, COL_DOWN = (0, 0, 1), (0, 0, -1)
NEIGHBOURS = (
    FRAME_UP, FRAME_DOWN, ROW_UP, ROW_DOWN, COL_UP, COL_DOWN,
    (1, -1, 0), (-1, 1, 0), (1, 0, -1), (-1, 0, 1), (0, 1, -1), (0, -1, 1),
)

CUTS = (5, 11)
STEPS = len(CUTS) + 1


def spans(first, back, *more):
    edges = [first] + [cut - back for cut in CUTS] + [16]
    out = [[(a, b)] if b > a else [] for a, b in zip(edges, edges[1:])]
    out[-1] += more
    return out


CHUNKS = (spans(0, -1), spans(0, 0), spans(1, 1, (0, 1)))
DUAL_STEPS = (spans(0, 0), spans(0, 1), spans(1, 2, (0, 1)))
PRIMAL_STEPS = (spans(0, 0), spans(1, 1, (0, 1)), spans(2, 2, (0, 2)))
PHASES = (("x", "tm", "core"), ("row",))
ABOVE_STEP = (0, STEPS - 1, STEPS - 1)
LOW_CHUNK = (STEPS - 1, 0, STEPS - 1)

UNROLL = 4
PACK_UNROLL = 16


def grouped(g0, g1, body, carry, unroll):
    steps = (g1 - g0) // unroll

    def step(i, carry):
        for u in range(unroll):
            carry = body(g0 + i * unroll + u, carry)
        return carry

    if steps > 1:
        carry = lax.fori_loop(0, steps, step, carry)
    elif steps == 1:
        carry = step(0, carry)
    for g in range(g0 + steps * unroll, g1):
        carry = body(g, carry)
    return carry


def rows_of(group):
    start = 8 + 8 * group
    return pl.ds(start if isinstance(start, int) else pl.multiple_of(start, 8), 8)


def kernel(
    sizes, f_hbm, fid_hbm, out_v, gaps_ref,
    ub, p, gu, res, damp, inv_fid, fid, c0, c255, cn, cp, tcn, tcp, rcn, rcp, pc, part, by_phase0, by_phase1, by_phase2,
    load_sem,
    fr_send, fr_recv, row_send, row_recv, col_send, col_recv, tr_send, tr_recv, tc_send, tc_recv, rc_send, rc_recv,
    ar_send, ar_recv, token_sem,
):
    n_tm, n_row, n_col = sizes
    by_phase = (by_phase0, by_phase1, by_phase2)
    at = (lax.axis_index("tm"), lax.axis_index("row"), lax.axis_index("col"))

    def there(step):
        return dict(tm=at[0] + step[0], row=at[1] + step[1], col=at[2] + step[2])

    def exists(step):
        found = None
        for pos, size, move in zip(at, sizes, step):
            if move:
                ok = pos < size - 1 if move > 0 else pos > 0
                found = ok if found is None else jnp.logical_and(found, ok)
        return found

    lane = lax.broadcasted_iota(jnp.int32, (8, 128), 1)
    sublane = lax.broadcasted_iota(jnp.int32, (8, 128), 0)
    first_lane, last_lane = lane == 0, lane == 127
    first_row, first_col, first_tm = at[1] == 0, at[2] == 0, at[0] == 0
    last_row, last_col, last_tm = at[1] == n_row - 1, at[2] == n_col - 1, at[0] == n_tm - 1
    edge_lane = jnp.logical_and(last_lane, last_col)

    frame_loads, fid_loads = {}, []
    for h in range(2):
        cols = pl.ds(128 * h, 128)
        for t in range(4):
            frame_loads[t, h] = pltpu.make_async_copy(
                f_hbm.at[t, :, cols], ub.at[0, t + 1, h, 8:136, :], load_sem.at[t, h])
        fid_loads.append(pltpu.make_async_copy(fid_hbm.at[:, :, cols], fid.at[:, h], load_sem.at[4, h]))
    for t in (0, 3, 1, 2):
        for h in range(2):
            frame_loads[t, h].start()
    for load in fid_loads:
        load.start()

    def ring(**moves):
        out = {}
        for name, pos, size in zip(("tm", "row", "col"), at, sizes):
            out[name] = lax.rem(pos + (moves.get(name, 0) + size), size)
        return out

    barrier = pltpu.get_barrier_semaphore()
    arrivals = 0
    for move in NEIGHBOURS:
        if sum(map(abs, move)) == 1:
            pl.semaphore_signal(
                barrier, inc=1, device_id=ring(tm=move[0], row=move[1], col=move[2]), device_id_type=MESH)
            arrivals = arrivals + 1
            continue
        ok = exists(move)

        @pl.when(ok)
        def _():
            pl.semaphore_signal(barrier, inc=1, device_id=there(move), device_id_type=MESH)

        arrivals = arrivals + ok.astype(jnp.int32)

    def tokens(name, count):
        reach, out = 1, []
        while 2 * reach < count:
            out.append((name, reach))
            reach *= 2
        return out

    of_rows, of_cols = tokens("row", n_row), tokens("col", n_col)
    rounds = list(zip_longest(of_rows, of_cols + [("tm", 1)] * (n_tm // 2)))

    def tell(i):
        for j, token in enumerate(rounds[i] if i < len(rounds) else ()):
            if token:
                name, reach = token
                for d in (reach, -reach):
                    pl.semaphore_signal(
                        token_sem.at[i, j], inc=1, device_id=ring(**{name: d}), device_id_type=MESH)

    def hear(i):
        for j, token in enumerate(rounds[i] if i < len(rounds) else ()):
            if token:
                pl.semaphore_wait(token_sem.at[i, j], 2)

    zero = jnp.zeros((8, 128), F32)

    @pl.when(first_row)
    def _():
        for t in range(1, 5):
            for h in range(2):
                p[1, t, h, 0:8, :] = zero

    def remote(src, dst, send, recv, step):
        return pltpu.make_async_remote_copy(
            src_ref=src, dst_ref=dst, send_sem=send, recv_sem=recv, device_id=there(step), device_id_type=MESH
        )

    def frame_copies(k, c):
        out = []
        for i, (move, src, dst) in enumerate(((FRAME_DOWN, 1, 5), (FRAME_UP, 4, 0))):
            for j, (g0, g1) in enumerate(CHUNKS[k][c]):
                rows = pl.ds(8 + 8 * g0, 8 * (g1 - g0))
                out.append((move, remote(
                    ub.at[k, src, :, rows, :], ub.at[k, dst, :, rows, :],
                    fr_send.at[k, c, i, j], fr_recv.at[k, c, i, j], move)))
        return out

    low, high, ghost_low, ghost_high = pl.ds(8, 1), pl.ds(135, 1), pl.ds(7, 1), pl.ds(136, 1)

    def low_copies(k):
        c = LOW_CHUNK[k]
        return [
            (ROW_DOWN, remote(
                ub.at[k, 1:5, :, low, :], ub.at[k, 1:5, :, ghost_high, :], row_send.at[k, 0], row_recv.at[k, 0], ROW_DOWN)),
            ((1, -1, 0), remote(
                ub.at[k, 4, :, low, :], ub.at[k, 0, :, ghost_high, :], tr_send.at[k, 0], tr_recv.at[k, 0], (1, -1, 0))),
            ((0, -1, 1), remote(c255.at[k, c], rcp.at[k], rc_send.at[k, 1], rc_recv.at[k, 1], (0, -1, 1))),
        ]

    def high_copies(k):
        c = STEPS - 1
        return [
            (ROW_UP, remote(
                ub.at[k, 1:5, :, high, :], ub.at[k, 1:5, :, ghost_low, :], row_send.at[k, 1], row_recv.at[k, 1], ROW_UP)),
            ((-1, 1, 0), remote(
                ub.at[k, 1, :, high, :], ub.at[k, 5, :, ghost_low, :], tr_send.at[k, 1], tr_recv.at[k, 1], (-1, 1, 0))),
            ((0, 1, -1), remote(c0.at[k, c], rcn.at[k], rc_send.at[k, 0], rc_recv.at[k, 0], (0, 1, -1))),
        ]

    def col_copies(k, c):
        return [
            (COL_DOWN, remote(c0.at[k, c], cn.at[k, c], col_send.at[k, c, 0], col_recv.at[k, c, 0], COL_DOWN)),
            (COL_UP, remote(c255.at[k, c], cp.at[k, c], col_send.at[k, c, 1], col_recv.at[k, c, 1], COL_UP)),
            ((1, 0, -1), remote(c0.at[k, c], tcn.at[k, c], tc_send.at[k, c, 0], tc_recv.at[k, c, 0], (1, 0, -1))),
            ((-1, 0, 1), remote(c255.at[k, c], tcp.at[k, c], tc_send.at[k, c, 1], tc_recv.at[k, c, 1], (-1, 0, 1))),
        ]

    def start(copies):
        for step, copy in copies:
            @pl.when(exists(step))
            def _():
                copy.start()

    def wait_sent(copies):
        for step, copy in copies:
            @pl.when(exists(step))
            def _():
                copy.wait_send()

    def wait_received(copies):
        for step, copy in copies:
            @pl.when(exists(tuple(-s for s in step)))
            def _():
                copy.wait_recv()

    def col_chunks(k):
        return range(STEPS) if k else range(STEPS - 1, STEPS)

    def all_copies(k):
        out = low_copies(k) + high_copies(k)
        for c in range(STEPS):
            out += frame_copies(k, c)
        for c in col_chunks(k):
            out += col_copies(k, c)
        return out

    def packed_at(t, g):
        return (t - 1) * 16 + g

    def packed(x0, x1, t, g, held):
        i = packed_at(t, g)
        here = lane == i
        return (
            jnp.where(here, pltpu.roll(x0, i, 1), held[0]),
            jnp.where(here, pltpu.roll(x1, i + 1, 1), held[1]),
        )

    def pack(k, g0, g1, held):
        def body(g, held):
            for t in range(1, 5):
                held = packed(ub[k, t, 0, rows_of(g), :], ub[k, t, 1, rows_of(g), :], t, g, held)
            return held

        return grouped(g0, g1, body, held, PACK_UNROLL)

    def project(k, m, g):
        if k == 0:
            square = g[0] * g[0] + g[1] * g[1] + g[2] * g[2]
            root = lax.rsqrt(jnp.maximum(square, TINY))
            scale = jnp.minimum(SIGMA, root)
            return [g[d] * scale for d in range(3)], square * root
        square = m[0] * m[0] + m[1] * m[1] + m[2] * m[2]
        scale = lax.rsqrt(jnp.maximum(square, 1.0))
        return [m[d] * scale for d in range(3)], None

    def dual_group(k, rows, below, frames, ghost_of, total):
        x = [[ub[k, t, h, rows, :] for h in range(2)] for t in range(frames[0], 6)]
        for t in frames:
            here, later = x[t - frames[0]], x[t - frames[0] + 1]
            if t == 4:
                later = [jnp.where(last_tm, here[h], later[h]) for h in range(2)]
            rolled = [pltpu.roll(here[h], 127, 1) for h in range(2)]
            after = [
                jnp.where(last_lane, rolled[1], rolled[0]),
                jnp.where(edge_lane, here[1], jnp.where(last_lane, ghost_of(t), rolled[1])),
            ]
            for h in range(2):
                g = [later[h] - here[h], ub[k, t, h, below, :] - here[h], after[h] - here[h]]
                m = None if k == 0 else [p[d, t, h, rows, :] + SIGMA * g[d] for d in range(3)]
                new, length = project(k, m, g)
                if t == 0:
                    new[0] = jnp.where(first_tm, 0.0, new[0])
                for d in range(3):
                    p[d, t, h, rows, :] = new[d]
                if total is None or t == 0:
                    continue
                if k == 0:
                    for d in range(3):
                        gu[d, t - 1, h, pl.ds(rows.start - 8, 8), :] = g[d]
                    total = total + length
                else:
                    own = pl.ds(rows.start - 8, 8)
                    if k == 1:
                        s = [g[d] + gu[d, t - 1, h, own, :] for d in range(3)]
                        for d in range(3):
                            gu[d, t - 1, h, own, :] = s[d]
                    else:
                        s = [g[d] + 0.5 * gu[d, t - 1, h, own, :] for d in range(3)]
                    square = s[0] * s[0] + s[1] * s[1] + s[2] * s[2]
                    total = total + square * lax.rsqrt(jnp.maximum(square, TINY))
        return total

    def dual_range(k, b, g0, g1, total):
        def body(g, total):
            rows = rows_of(g)
            nexts, frame_nexts = cn[k, b], tcn[k, b]

            def ghost_of(t):
                if t == 0:
                    return pltpu.roll(frame_nexts, 127 - packed_at(4, g), 1)
                return pltpu.roll(nexts, 127 - packed_at(t, g), 1)

            return dual_group(k, rows, pl.ds(rows.start + 1, 8), range(5), ghost_of, total)

        return grouped(g0, g1, body, total, UNROLL)

    def dual_above(k):
        @pl.when(jnp.logical_not(first_row))
        def _():
            nexts = rcn[k]
            dual_group(
                k, pl.ds(0, 8), pl.ds(1, 8), range(1, 5),
                lambda t: pltpu.roll(nexts, 127 - packed_at(t, 15), 1), None,
            )

    def dual_left(k, b, last):
        here, later_left = cp[k, b], tcp[k, b]
        later = jnp.where(lane >= 48, pltpu.roll(later_left, 48, 1), pltpu.roll(here, 112, 1))
        later = jnp.where(jnp.logical_and(lane >= 48, last_tm), here, later)
        last_group = jnp.bitwise_and(lane, 15) == 15
        follow = pltpu.roll(here, 127, 1)
        if last:
            follow = jnp.where(last_group, pltpu.roll(rcp[k], 15, 1), follow)
        below = jnp.where(sublane == 7, pltpu.roll(follow, 7, 0), pltpu.roll(here, 7, 0))
        bottom = jnp.logical_and(jnp.logical_and(sublane == 7, last_group), last_row)
        below = jnp.where(bottom, here, below)
        g = [later - here, below - here, c0[k, b] - here]
        m = None if k == 0 else [pc[k, d] + SIGMA * g[d] for d in range(3)]
        new, _ = project(k, m, g)
        for d in range(3):
            pc[k + 1, d] = new[d]
        pc[k + 1, 3] = jnp.where(first_col, 0.0, new[2])

    def primal_range(k, g0, g1, total):
        def body(g, total):
            rows = rows_of(g)
            own = pl.ds(rows.start - 8, 8)
            before_rows = pl.ds(rows.start - 1, 8)
            left = pc[k + 1, 3]
            for t in range(1, 5):
                q = [p[2, t, h, rows, :] for h in range(2)]
                rolled = [pltpu.roll(q[h], 1, 1) for h in range(2)]
                ghost = pltpu.roll(left, 128 - packed_at(t, g), 1)
                before = [jnp.where(first_lane, ghost, rolled[0]), jnp.where(first_lane, rolled[0], rolled[1])]
                for h in range(2):
                    e = (
                        (p[0, t, h, rows, :] - p[0, t - 1, h, rows, :])
                        + (p[1, t, h, rows, :] - p[1, t, h, before_rows, :])
                        + (q[h] - before[h])
                    )
                    f = ub[0, t, h, rows, :]
                    scale = damp[t - 1, h, own, :]
                    total = total + (e * e * inv_fid[t - 1, h, own, :] + f * e)
                    if k == 0:
                        new = scale * (TAU * e)
                        bar = f + 2.0 * new
                    else:
                        old = res[t - 1, h, own, :]
                        total = total + old * old * fid[t - 1, h, own, :]
                        new = scale * (old + TAU * e)
                        bar = f + (2.0 * new - old)
                    if k < ITERS - 1:
                        res[t - 1, h, own, :] = new
                        ub[k + 1, t, h, rows, :] = bar
                    else:
                        out_v[t - 1, h, own, :] = f + new
            return total

        return grouped(g0, g1, body, total, UNROLL)

    def weights():
        for load in fid_loads:
            load.wait()

        @pl.loop(0, GROUPS)
        def _(g):
            own = pl.ds(pl.multiple_of(8 * g, 8), 8)
            for t in range(4):
                for h in range(2):
                    lam = fid[t, h, own, :]
                    damp[t, h, own, :] = 1.0 / (1.0 + TAU * lam)
                    inv_fid[t, h, own, :] = 0.5 / lam
                    fid[t, h, own, :] = 0.5 * lam

    for load in frame_loads.values():
        load.wait()
    c0[0, STEPS - 1], c255[0, STEPS - 1] = pack(0, 0, GROUPS, (zero, zero))
    pl.semaphore_wait(barrier, arrivals)
    start(col_copies(0, STEPS - 1))
    start(frame_copies(0, 0))
    start(low_copies(0) + high_copies(0))
    tell(0)
    for c in range(1, STEPS):
        start(frame_copies(0, c))
    weights()
    hear(0)
    tell(1)

    row = jnp.zeros((1, 128), F32)
    row_lane = lax.broadcasted_iota(jnp.int32, (1, 128), 1)
    for k in range(ITERS):
        length, total, held = zero, zero, (zero, zero)
        for c in range(STEPS):
            final = c == STEPS - 1
            b = c if k else STEPS - 1
            wait_received(frame_copies(k, c))
            if k or c == 0:
                wait_received(col_copies(k, b))
            if c == ABOVE_STEP[k]:
                wait_received(high_copies(k))
                dual_above(k)
            if final:
                wait_received(low_copies(k))
                hear(k + 1)
                tell(k + 2)

                @pl.when(last_row)
                def _():
                    for t in range(5):
                        for h in range(2):
                            ub[k, t, h, 136:137, :] = ub[k, t, h, 135:136, :]

            dual_left(k, b, final)
            for span in DUAL_STEPS[k][c]:
                length = dual_range(k, b, *span, length)
            for span in PRIMAL_STEPS[k][c]:
                total = primal_range(k, *span, total)
            if k == ITERS - 1:
                continue
            for span in CHUNKS[k + 1][c]:
                held = pack(k + 1, *span, held)
            c0[k + 1, c], c255[k + 1, c] = held
            start(col_copies(k + 1, c))
            if c == LOW_CHUNK[k + 1]:
                start(low_copies(k + 1))
            if final:
                start(high_copies(k + 1))
            start(frame_copies(k + 1, c))
        share = jnp.sum(total + (1.0 if k == 0 else 0.5) * length, axis=0, keepdims=True)
        row = jnp.where(row_lane == k, jnp.sum(share, axis=1, keepdims=True), row)

    places = {"tm": (at[0], n_tm), "row": (at[1], n_row), "x": (at[2] // 2, n_col // 2), "core": (at[2] % 2, 2)}

    def exchange(i, axes, row):
        slots, count, me = by_phase[i], 1, 0
        for name in axes:
            pos, size = places[name]
            count, me = count * size, me * size + pos
        part[i] = row
        slots[me] = row

        def tell_one(j):
            there, left = {name: places[name][0] for name in places}, j
            for name in reversed(axes):
                size = places[name][1]
                off = jnp.bitwise_and(left, size - 1)
                there[name] = jnp.bitwise_and(there[name] + off, size - 1) if axes == ("row",) else jnp.bitwise_xor(there[name], off)
                left = jnp.right_shift(left, size.bit_length() - 1)
            pltpu.make_async_remote_copy(
                src_ref=part.at[i], dst_ref=slots.at[me], send_sem=ar_send.at[i], recv_sem=ar_recv.at[i],
                device_id=dict(tm=there["tm"], row=there["row"], col=there["x"] * 2 + there["core"]),
                device_id_type=MESH,
            ).start()

        if axes == ("row",):
            for j in sorted(range(1, count), key=lambda j: -min(j, count - j)):
                tell_one(j)
        else:
            pl.loop(1, count)(lambda j: tell_one(count - j))

        if i == 0:
            for k in range(ITERS):
                wait_sent(all_copies(k))
        landed = slots.at[pl.ds(0, count - 1)]
        pltpu.make_async_copy(landed, landed, ar_recv.at[i]).wait()
        got = [slots[j] for j in range(count)]
        while len(got) > 1:
            got = [got[j] + got[j + 1] for j in range(0, len(got), 2)]
        return got[0]

    def drain(i, axes):
        count = 1
        for name in axes:
            count *= places[name][1]
        landed = by_phase[i].at[pl.ds(0, count - 1)]
        pltpu.make_async_copy(landed, landed, ar_send.at[i]).wait()

    for i, axes in enumerate(PHASES):
        row = exchange(i, axes, row)
    cells = float(4 * 128 * 256) * float(n_tm * n_row * n_col)
    gaps_ref[...] = row * (1.0 / cells)

    for i, axes in enumerate(PHASES):
        drain(i, axes)


def put_out(out_v, gaps_ref, out_hbm, gaps_out, sem, gaps_s):
    puts = [pltpu.make_async_copy(out_v.at[:, h], out_hbm.at[:, :, pl.ds(128 * h, 128)], sem.at[h]) for h in range(2)]
    for put in puts:
        put.start()
    for k in range(ITERS):
        gaps_s[k] = gaps_ref[0, k]
    last = pltpu.make_async_copy(gaps_s, gaps_out, sem.at[2])
    last.start()
    puts.append(last)
    for put in puts:
        put.wait()


def on_device(sizes, noisy_video, fidelity):
    n_chunks = STEPS
    dma = pltpu.SemaphoreType.DMA
    vmem = lambda *shape: pltpu.VMEM(shape, F32)
    out, gaps = pl.pallas_call(
        functools.partial(kernel, sizes),
        out_shape=(vmem(4, 2, 128, 128), vmem(1, 128)),
        in_specs=[pl.BlockSpec(memory_space=pl.ANY)] * 2,
        out_specs=(pl.BlockSpec(memory_space=pltpu.VMEM), pl.BlockSpec(memory_space=pltpu.VMEM)),
        scratch_shapes=[
            vmem(3, 6, 2, 144, 128),
            vmem(3, 5, 2, 136, 128),
            vmem(3, 4, 2, 128, 128),
            vmem(4, 2, 128, 128),
            vmem(4, 2, 128, 128),
            vmem(4, 2, 128, 128),
            vmem(4, 2, 128, 128),
            vmem(3, n_chunks, 8, 128),
            vmem(3, n_chunks, 8, 128),
            vmem(3, n_chunks, 8, 128),
            vmem(3, n_chunks, 8, 128),
            vmem(3, n_chunks, 8, 128),
            vmem(3, n_chunks, 8, 128),
            vmem(3, 8, 128),
            vmem(3, 8, 128),
            vmem(4, 4, 8, 128),
            vmem(3, 1, 128),
            vmem(64, 1, 128),
            vmem(64, 1, 128),
            vmem(64, 1, 128),
            dma((5, 2)),
            dma((3, n_chunks, 2, 2)), dma((3, n_chunks, 2, 2)),
            dma((3, 2)), dma((3, 2)),
            dma((3, n_chunks, 2)), dma((3, n_chunks, 2)),
            dma((3, 2)), dma((3, 2)),
            dma((3, n_chunks, 2)), dma((3, n_chunks, 2)),
            dma((3, 2)), dma((3, 2)),
            dma((3,)), dma((3,)),
            pltpu.SemaphoreType.REGULAR((4, 3)),
        ],
        compiler_params=pltpu.CompilerParams(collective_id=0, has_side_effects=True),
    )(noisy_video, fidelity)
    return pl.pallas_call(
        put_out,
        out_shape=(jax.ShapeDtypeStruct(noisy_video.shape, F32), jax.ShapeDtypeStruct((ITERS,), F32)),
        in_specs=[pl.BlockSpec(memory_space=pltpu.VMEM)] * 2,
        out_specs=(pl.BlockSpec(memory_space=pl.ANY), pl.BlockSpec(memory_space=pl.ANY)),
        scratch_shapes=[dma((3,)), pltpu.SMEM((ITERS,), F32)],
    )(*(pltpu.with_memory_space_constraint(x, pltpu.VMEM) for x in (out, gaps)))


def solution(mesh):
    sizes = (mesh.shape["tm"], mesh.shape["row"], mesh.shape["col"])
    placed = P("tm", "row", "col")
    return jax.shard_map(
        functools.partial(on_device, sizes),
        mesh=mesh,
        in_specs=(placed, placed),
        out_specs=(placed, P()),
        check_vma=False,
    )
```

```python
import functools
from itertools import zip_longest

import jax
import jax.numpy as jnp
from jax import lax
from jax.experimental import pallas as pl
from jax.experimental.pallas import tpu as pltpu
from jax.sharding import PartitionSpec as P

ITERS = 3
SIGMA = 0.28
TAU = 0.28
TINY = 1.1754943508222875e-38
MESH = pl.DeviceIdType.MESH
F32 = jnp.float32

GROUPS = 16

FRAME_UP, FRAME_DOWN = (1, 0, 0), (-1, 0, 0)
ROW_UP, ROW_DOWN = (0, 1, 0), (0, -1, 0)
COL_UP, COL_DOWN = (0, 0, 1), (0, 0, -1)
NEIGHBOURS = (
    FRAME_UP, FRAME_DOWN, ROW_UP, ROW_DOWN, COL_UP, COL_DOWN,
    (1, -1, 0), (-1, 1, 0), (1, 0, -1), (-1, 0, 1), (0, 1, -1), (0, -1, 1),
)

CUTS = (5, 11)
STEPS = len(CUTS) + 1


def spans(first, back, *more):
    edges = [first] + [cut - back for cut in CUTS] + [16]
    out = [[(a, b)] if b > a else [] for a, b in zip(edges, edges[1:])]
    out[-1] += more
    return out


CHUNKS = (spans(0, -1), spans(0, 0), spans(1, 1, (0, 1)))
DUAL_STEPS = (spans(0, 0), spans(0, 1), spans(1, 2, (0, 1)))
PRIMAL_STEPS = (spans(0, 0), spans(1, 1, (0, 1)), spans(2, 2, (0, 2)))
PHASES = (("x", "tm", "core"), ("row",))
ABOVE_STEP = (0, STEPS - 1, STEPS - 1)
LOW_CHUNK = (STEPS - 1, 0, STEPS - 1)

UNROLL = 6
PACK_UNROLL = 16


def grouped(g0, g1, body, carry, unroll):
    steps = (g1 - g0) // unroll

    def step(i, carry):
        for u in range(unroll):
            carry = body(g0 + i * unroll + u, carry)
        return carry

    if steps > 1:
        carry = lax.fori_loop(0, steps, step, carry)
    elif steps == 1:
        carry = step(0, carry)
    for g in range(g0 + steps * unroll, g1):
        carry = body(g, carry)
    return carry


def rows_of(group):
    start = 8 + 8 * group
    return pl.ds(start if isinstance(start, int) else pl.multiple_of(start, 8), 8)


def kernel(
    sizes, f_hbm, fid_hbm, out_v, gaps_ref,
    ub, p, gu, res, damp, inv_fid, fid, c0, c255, cn, cp, tcn, tcp, rcn, rcp, pc, part, by_phase0, by_phase1, by_phase2,
    load_sem,
    fr_send, fr_recv, row_send, row_recv, col_send, col_recv, tr_send, tr_recv, tc_send, tc_recv, rc_send, rc_recv,
    ar_send, ar_recv, token_sem,
):
    n_tm, n_row, n_col = sizes
    by_phase = (by_phase0, by_phase1, by_phase2)
    at = (lax.axis_index("tm"), lax.axis_index("row"), lax.axis_index("col"))

    def there(step):
        return dict(tm=at[0] + step[0], row=at[1] + step[1], col=at[2] + step[2])

    def exists(step):
        found = None
        for pos, size, move in zip(at, sizes, step):
            if move:
                ok = pos < size - 1 if move > 0 else pos > 0
                found = ok if found is None else jnp.logical_and(found, ok)
        return found

    lane = lax.broadcasted_iota(jnp.int32, (8, 128), 1)
    sublane = lax.broadcasted_iota(jnp.int32, (8, 128), 0)
    first_lane, last_lane = lane == 0, lane == 127
    first_row, first_col, first_tm = at[1] == 0, at[2] == 0, at[0] == 0
    last_row, last_col, last_tm = at[1] == n_row - 1, at[2] == n_col - 1, at[0] == n_tm - 1
    edge_lane = jnp.logical_and(last_lane, last_col)

    frame_loads, fid_loads = {}, []
    for h in range(2):
        cols = pl.ds(128 * h, 128)
        for t in range(4):
            frame_loads[t, h] = pltpu.make_async_copy(
                f_hbm.at[t, :, cols], ub.at[0, t + 1, h, 8:136, :], load_sem.at[t, h])
        fid_loads.append(pltpu.make_async_copy(fid_hbm.at[:, :, cols], fid.at[:, h], load_sem.at[4, h]))
    for t in (0, 3, 1, 2):
        for h in range(2):
            frame_loads[t, h].start()
    for load in fid_loads:
        load.start()

    def ring(**moves):
        out = {}
        for name, pos, size in zip(("tm", "row", "col"), at, sizes):
            out[name] = lax.rem(pos + (moves.get(name, 0) + size), size)
        return out

    barrier = pltpu.get_barrier_semaphore()
    arrivals = 0
    for move in NEIGHBOURS:
        if sum(map(abs, move)) == 1:
            pl.semaphore_signal(
                barrier, inc=1, device_id=ring(tm=move[0], row=move[1], col=move[2]), device_id_type=MESH)
            arrivals = arrivals + 1
            continue
        ok = exists(move)

        @pl.when(ok)
        def _():
            pl.semaphore_signal(barrier, inc=1, device_id=there(move), device_id_type=MESH)

        arrivals = arrivals + ok.astype(jnp.int32)

    def tokens(name, count):
        reach, out = 1, []
        while 2 * reach < count:
            out.append((name, reach))
            reach *= 2
        return out

    of_rows, of_cols = tokens("row", n_row), tokens("col", n_col)
    rounds = list(zip_longest(of_rows, of_cols + [("tm", 1)] * (n_tm // 2)))

    def tell(i):
        for j, token in enumerate(rounds[i] if i < len(rounds) else ()):
            if token:
                name, reach = token
                for d in (reach, -reach):
                    pl.semaphore_signal(
                        token_sem.at[i, j], inc=1, device_id=ring(**{name: d}), device_id_type=MESH)

    def hear(i):
        for j, token in enumerate(rounds[i] if i < len(rounds) else ()):
            if token:
                pl.semaphore_wait(token_sem.at[i, j], 2)

    zero = jnp.zeros((8, 128), F32)

    @pl.when(first_row)
    def _():
        for t in range(1, 5):
            for h in range(2):
                p[1, t, h, 0:8, :] = zero

    def remote(src, dst, send, recv, step):
        return pltpu.make_async_remote_copy(
            src_ref=src, dst_ref=dst, send_sem=send, recv_sem=recv, device_id=there(step), device_id_type=MESH
        )

    def frame_copies(k, c):
        out = []
        for i, (move, src, dst) in enumerate(((FRAME_DOWN, 1, 5), (FRAME_UP, 4, 0))):
            for j, (g0, g1) in enumerate(CHUNKS[k][c]):
                rows = pl.ds(8 + 8 * g0, 8 * (g1 - g0))
                out.append((move, remote(
                    ub.at[k, src, :, rows, :], ub.at[k, dst, :, rows, :],
                    fr_send.at[k, c, i, j], fr_recv.at[k, c, i, j], move)))
        return out

    low, high, ghost_low, ghost_high = pl.ds(8, 1), pl.ds(135, 1), pl.ds(7, 1), pl.ds(136, 1)

    def low_copies(k):
        c = LOW_CHUNK[k]
        return [
            (ROW_DOWN, remote(
                ub.at[k, 1:5, :, low, :], ub.at[k, 1:5, :, ghost_high, :], row_send.at[k, 0], row_recv.at[k, 0], ROW_DOWN)),
            ((1, -1, 0), remote(
                ub.at[k, 4, :, low, :], ub.at[k, 0, :, ghost_high, :], tr_send.at[k, 0], tr_recv.at[k, 0], (1, -1, 0))),
            ((0, -1, 1), remote(c255.at[k, c], rcp.at[k], rc_send.at[k, 1], rc_recv.at[k, 1], (0, -1, 1))),
        ]

    def high_copies(k):
        c = STEPS - 1
        return [
            (ROW_UP, remote(
                ub.at[k, 1:5, :, high, :], ub.at[k, 1:5, :, ghost_low, :], row_send.at[k, 1], row_recv.at[k, 1], ROW_UP)),
            ((-1, 1, 0), remote(
                ub.at[k, 1, :, high, :], ub.at[k, 5, :, ghost_low, :], tr_send.at[k, 1], tr_recv.at[k, 1], (-1, 1, 0))),
            ((0, 1, -1), remote(c0.at[k, c], rcn.at[k], rc_send.at[k, 0], rc_recv.at[k, 0], (0, 1, -1))),
        ]

    def col_copies(k, c):
        return [
            (COL_DOWN, remote(c0.at[k, c], cn.at[k, c], col_send.at[k, c, 0], col_recv.at[k, c, 0], COL_DOWN)),
            (COL_UP, remote(c255.at[k, c], cp.at[k, c], col_send.at[k, c, 1], col_recv.at[k, c, 1], COL_UP)),
            ((1, 0, -1), remote(c0.at[k, c], tcn.at[k, c], tc_send.at[k, c, 0], tc_recv.at[k, c, 0], (1, 0, -1))),
            ((-1, 0, 1), remote(c255.at[k, c], tcp.at[k, c], tc_send.at[k, c, 1], tc_recv.at[k, c, 1], (-1, 0, 1))),
        ]

    def start(copies):
        for step, copy in copies:
            @pl.when(exists(step))
            def _():
                copy.start()

    def wait_sent(copies):
        for step, copy in copies:
            @pl.when(exists(step))
            def _():
                copy.wait_send()

    def wait_received(copies):
        for step, copy in copies:
            @pl.when(exists(tuple(-s for s in step)))
            def _():
                copy.wait_recv()

    def col_chunks(k):
        return range(STEPS) if k else range(STEPS - 1, STEPS)

    def all_copies(k):
        out = low_copies(k) + high_copies(k)
        for c in range(STEPS):
            out += frame_copies(k, c)
        for c in col_chunks(k):
            out += col_copies(k, c)
        return out

    def packed_at(t, g):
        return (t - 1) * 16 + g

    def packed(x0, x1, t, g, held):
        i = packed_at(t, g)
        here = lane == i
        return (
            jnp.where(here, pltpu.roll(x0, i, 1), held[0]),
            jnp.where(here, pltpu.roll(x1, i + 1, 1), held[1]),
        )

    def pack(k, g0, g1, held):
        def body(g, held):
            for t in range(1, 5):
                held = packed(ub[k, t, 0, rows_of(g), :], ub[k, t, 1, rows_of(g), :], t, g, held)
            return held

        return grouped(g0, g1, body, held, PACK_UNROLL)

    def project(k, m, g):
        if k == 0:
            square = g[0] * g[0] + g[1] * g[1] + g[2] * g[2]
            root = lax.rsqrt(jnp.maximum(square, TINY))
            scale = jnp.minimum(SIGMA, root)
            return [g[d] * scale for d in range(3)], square * root
        square = m[0] * m[0] + m[1] * m[1] + m[2] * m[2]
        scale = lax.rsqrt(jnp.maximum(square, 1.0))
        return [m[d] * scale for d in range(3)], None

    def dual_group(k, rows, below, frames, ghost_of, total):
        x = [[ub[k, t, h, rows, :] for h in range(2)] for t in range(frames[0], 6)]
        for t in frames:
            here, later = x[t - frames[0]], x[t - frames[0] + 1]
            if t == 4:
                later = [jnp.where(last_tm, here[h], later[h]) for h in range(2)]
            rolled = [pltpu.roll(here[h], 127, 1) for h in range(2)]
            after = [
                jnp.where(last_lane, rolled[1], rolled[0]),
                jnp.where(edge_lane, here[1], jnp.where(last_lane, ghost_of(t), rolled[1])),
            ]
            for h in range(2):
                g = [later[h] - here[h], ub[k, t, h, below, :] - here[h], after[h] - here[h]]
                m = None if k == 0 else [p[d, t, h, rows, :] + SIGMA * g[d] for d in range(3)]
                new, length = project(k, m, g)
                if t == 0:
                    new[0] = jnp.where(first_tm, 0.0, new[0])
                for d in range(3):
                    p[d, t, h, rows, :] = new[d]
                if total is None or t == 0:
                    continue
                if k == 0:
                    for d in range(3):
                        gu[d, t - 1, h, pl.ds(rows.start - 8, 8), :] = g[d]
                    total = total + length
                else:
                    own = pl.ds(rows.start - 8, 8)
                    if k == 1:
                        s = [g[d] + gu[d, t - 1, h, own, :] for d in range(3)]
                        for d in range(3):
                            gu[d, t - 1, h, own, :] = s[d]
                    else:
                        s = [g[d] + 0.5 * gu[d, t - 1, h, own, :] for d in range(3)]
                    square = s[0] * s[0] + s[1] * s[1] + s[2] * s[2]
                    total = total + square * lax.rsqrt(jnp.maximum(square, TINY))
        return total

    def dual_range(k, b, g0, g1, total):
        def body(g, total):
            rows = rows_of(g)
            nexts, frame_nexts = cn[k, b], tcn[k, b]

            def ghost_of(t):
                if t == 0:
                    return pltpu.roll(frame_nexts, 127 - packed_at(4, g), 1)
                return pltpu.roll(nexts, 127 - packed_at(t, g), 1)

            return dual_group(k, rows, pl.ds(rows.start + 1, 8), range(5), ghost_of, total)

        return grouped(g0, g1, body, total, UNROLL)

    def dual_above(k):
        @pl.when(jnp.logical_not(first_row))
        def _():
            nexts = rcn[k]
            dual_group(
                k, pl.ds(0, 8), pl.ds(1, 8), range(1, 5),
                lambda t: pltpu.roll(nexts, 127 - packed_at(t, 15), 1), None,
            )

    def dual_left(k, b, last):
        here, later_left = cp[k, b], tcp[k, b]
        later = jnp.where(lane >= 48, pltpu.roll(later_left, 48, 1), pltpu.roll(here, 112, 1))
        later = jnp.where(jnp.logical_and(lane >= 48, last_tm), here, later)
        last_group = jnp.bitwise_and(lane, 15) == 15
        follow = pltpu.roll(here, 127, 1)
        if last:
            follow = jnp.where(last_group, pltpu.roll(rcp[k], 15, 1), follow)
        below = jnp.where(sublane == 7, pltpu.roll(follow, 7, 0), pltpu.roll(here, 7, 0))
        bottom = jnp.logical_and(jnp.logical_and(sublane == 7, last_group), last_row)
        below = jnp.where(bottom, here, below)
        g = [later - here, below - here, c0[k, b] - here]
        m = None if k == 0 else [pc[k, d] + SIGMA * g[d] for d in range(3)]
        new, _ = project(k, m, g)
        for d in range(3):
            pc[k + 1, d] = new[d]
        pc[k + 1, 3] = jnp.where(first_col, 0.0, new[2])

    def primal_range(k, g0, g1, total):
        def body(g, total):
            rows = rows_of(g)
            own = pl.ds(rows.start - 8, 8)
            before_rows = pl.ds(rows.start - 1, 8)
            left = pc[k + 1, 3]
            for t in range(1, 5):
                q = [p[2, t, h, rows, :] for h in range(2)]
                rolled = [pltpu.roll(q[h], 1, 1) for h in range(2)]
                ghost = pltpu.roll(left, 128 - packed_at(t, g), 1)
                before = [jnp.where(first_lane, ghost, rolled[0]), jnp.where(first_lane, rolled[0], rolled[1])]
                for h in range(2):
                    e = (
                        (p[0, t, h, rows, :] - p[0, t - 1, h, rows, :])
                        + (p[1, t, h, rows, :] - p[1, t, h, before_rows, :])
                        + (q[h] - before[h])
                    )
                    f = ub[0, t, h, rows, :]
                    scale = damp[t - 1, h, own, :]
                    total = total + (e * e * inv_fid[t - 1, h, own, :] + f * e)
                    if k == 0:
                        new = scale * (TAU * e)
                        bar = f + 2.0 * new
                    else:
                        old = res[t - 1, h, own, :]
                        total = total + old * old * fid[t - 1, h, own, :]
                        new = scale * (old + TAU * e)
                        bar = f + (2.0 * new - old)
                    if k < ITERS - 1:
                        res[t - 1, h, own, :] = new
                        ub[k + 1, t, h, rows, :] = bar
                    else:
                        out_v[t - 1, h, own, :] = f + new
            return total

        return grouped(g0, g1, body, total, UNROLL)

    def weights():
        for load in fid_loads:
            load.wait()

        @pl.loop(0, GROUPS)
        def _(g):
            own = pl.ds(pl.multiple_of(8 * g, 8), 8)
            for t in range(4):
                for h in range(2):
                    lam = fid[t, h, own, :]
                    damp[t, h, own, :] = 1.0 / (1.0 + TAU * lam)
                    inv_fid[t, h, own, :] = 0.5 / lam
                    fid[t, h, own, :] = 0.5 * lam

    for load in frame_loads.values():
        load.wait()
    c0[0, STEPS - 1], c255[0, STEPS - 1] = pack(0, 0, GROUPS, (zero, zero))
    pl.semaphore_wait(barrier, arrivals)
    start(col_copies(0, STEPS - 1))
    start(frame_copies(0, 0))
    start(low_copies(0) + high_copies(0))
    tell(0)
    for c in range(1, STEPS):
        start(frame_copies(0, c))
    weights()
    hear(0)
    tell(1)

    row = jnp.zeros((1, 128), F32)
    row_lane = lax.broadcasted_iota(jnp.int32, (1, 128), 1)
    for k in range(ITERS):
        length, total, held = zero, zero, (zero, zero)
        for c in range(STEPS):
            final = c == STEPS - 1
            b = c if k else STEPS - 1
            wait_received(frame_copies(k, c))
            if k or c == 0:
                wait_received(col_copies(k, b))
            if c == ABOVE_STEP[k]:
                wait_received(high_copies(k))
                dual_above(k)
            if final:
                wait_received(low_copies(k))
                hear(k + 1)
                tell(k + 2)

                @pl.when(last_row)
                def _():
                    for t in range(5):
                        for h in range(2):
                            ub[k, t, h, 136:137, :] = ub[k, t, h, 135:136, :]

            dual_left(k, b, final)
            for span in DUAL_STEPS[k][c]:
                length = dual_range(k, b, *span, length)
            for span in PRIMAL_STEPS[k][c]:
                total = primal_range(k, *span, total)
            if k == ITERS - 1:
                continue
            for span in CHUNKS[k + 1][c]:
                held = pack(k + 1, *span, held)
            c0[k + 1, c], c255[k + 1, c] = held
            start(col_copies(k + 1, c))
            if c == LOW_CHUNK[k + 1]:
                start(low_copies(k + 1))
            if final:
                start(high_copies(k + 1))
            start(frame_copies(k + 1, c))
        share = jnp.sum(total + (1.0 if k == 0 else 0.5) * length, axis=0, keepdims=True)
        row = jnp.where(row_lane == k, jnp.sum(share, axis=1, keepdims=True), row)

    places = {"tm": (at[0], n_tm), "row": (at[1], n_row), "x": (at[2] // 2, n_col // 2), "core": (at[2] % 2, 2)}

    def exchange(i, axes, row):
        slots, count, me = by_phase[i], 1, 0
        for name in axes:
            pos, size = places[name]
            count, me = count * size, me * size + pos
        part[i] = row
        slots[me] = row

        def tell_one(j):
            there, left = {name: places[name][0] for name in places}, j
            for name in reversed(axes):
                size = places[name][1]
                off = jnp.bitwise_and(left, size - 1)
                there[name] = jnp.bitwise_and(there[name] + off, size - 1) if axes == ("row",) else jnp.bitwise_xor(there[name], off)
                left = jnp.right_shift(left, size.bit_length() - 1)
            pltpu.make_async_remote_copy(
                src_ref=part.at[i], dst_ref=slots.at[me], send_sem=ar_send.at[i], recv_sem=ar_recv.at[i],
                device_id=dict(tm=there["tm"], row=there["row"], col=there["x"] * 2 + there["core"]),
                device_id_type=MESH,
            ).start()

        if axes == ("row",):
            for j in sorted(range(1, count), key=lambda j: -min(j, count - j)):
                tell_one(j)
        else:
            pl.loop(1, count)(lambda j: tell_one(count - j))

        if i == 0:
            for k in range(ITERS):
                wait_sent(all_copies(k))
        landed = slots.at[pl.ds(0, count - 1)]
        pltpu.make_async_copy(landed, landed, ar_recv.at[i]).wait()
        got = [slots[j] for j in range(count)]
        while len(got) > 1:
            got = [got[j] + got[j + 1] for j in range(0, len(got), 2)]
        return got[0]

    def drain(i, axes):
        count = 1
        for name in axes:
            count *= places[name][1]
        landed = by_phase[i].at[pl.ds(0, count - 1)]
        pltpu.make_async_copy(landed, landed, ar_send.at[i]).wait()

    for i, axes in enumerate(PHASES):
        row = exchange(i, axes, row)
    cells = float(4 * 128 * 256) * float(n_tm * n_row * n_col)
    gaps_ref[...] = row * (1.0 / cells)

    for i, axes in enumerate(PHASES):
        drain(i, axes)


def put_out(out_v, gaps_ref, out_hbm, gaps_out, sem, gaps_s):
    puts = [pltpu.make_async_copy(out_v.at[:, h], out_hbm.at[:, :, pl.ds(128 * h, 128)], sem.at[h]) for h in range(2)]
    for put in puts:
        put.start()
    for k in range(ITERS):
        gaps_s[k] = gaps_ref[0, k]
    last = pltpu.make_async_copy(gaps_s, gaps_out, sem.at[2])
    last.start()
    puts.append(last)
    for put in puts:
        put.wait()


def on_device(sizes, noisy_video, fidelity):
    n_chunks = STEPS
    dma = pltpu.SemaphoreType.DMA
    vmem = lambda *shape: pltpu.VMEM(shape, F32)
    out, gaps = pl.pallas_call(
        functools.partial(kernel, sizes),
        out_shape=(vmem(4, 2, 128, 128), vmem(1, 128)),
        in_specs=[pl.BlockSpec(memory_space=pl.ANY)] * 2,
        out_specs=(pl.BlockSpec(memory_space=pltpu.VMEM), pl.BlockSpec(memory_space=pltpu.VMEM)),
        scratch_shapes=[
            vmem(3, 6, 2, 144, 128),
            vmem(3, 5, 2, 136, 128),
            vmem(3, 4, 2, 128, 128),
            vmem(4, 2, 128, 128),
            vmem(4, 2, 128, 128),
            vmem(4, 2, 128, 128),
            vmem(4, 2, 128, 128),
            vmem(3, n_chunks, 8, 128),
            vmem(3, n_chunks, 8, 128),
            vmem(3, n_chunks, 8, 128),
            vmem(3, n_chunks, 8, 128),
            vmem(3, n_chunks, 8, 128),
            vmem(3, n_chunks, 8, 128),
            vmem(3, 8, 128),
            vmem(3, 8, 128),
            vmem(4, 4, 8, 128),
            vmem(3, 1, 128),
            vmem(64, 1, 128),
            vmem(64, 1, 128),
            vmem(64, 1, 128),
            dma((5, 2)),
            dma((3, n_chunks, 2, 2)), dma((3, n_chunks, 2, 2)),
            dma((3, 2)), dma((3, 2)),
            dma((3, n_chunks, 2)), dma((3, n_chunks, 2)),
            dma((3, 2)), dma((3, 2)),
            dma((3, n_chunks, 2)), dma((3, n_chunks, 2)),
            dma((3, 2)), dma((3, 2)),
            dma((3,)), dma((3,)),
            pltpu.SemaphoreType.REGULAR((4, 3)),
        ],
        compiler_params=pltpu.CompilerParams(collective_id=0, has_side_effects=True),
    )(noisy_video, fidelity)
    return pl.pallas_call(
        put_out,
        out_shape=(jax.ShapeDtypeStruct(noisy_video.shape, F32), jax.ShapeDtypeStruct((ITERS,), F32)),
        in_specs=[pl.BlockSpec(memory_space=pltpu.VMEM)] * 2,
        out_specs=(pl.BlockSpec(memory_space=pl.ANY), pl.BlockSpec(memory_space=pl.ANY)),
        scratch_shapes=[dma((3,)), pltpu.SMEM((ITERS,), F32)],
    )(*(pltpu.with_memory_space_constraint(x, pltpu.VMEM) for x in (out, gaps)))


def solution(mesh):
    sizes = (mesh.shape["tm"], mesh.shape["row"], mesh.shape["col"])
    placed = P("tm", "row", "col")
    return jax.shard_map(
        functools.partial(on_device, sizes),
        mesh=mesh,
        in_specs=(placed, placed),
        out_specs=(placed, P()),
        check_vma=False,
    )
```
